32 devices in a mesh: sub: 16 (over z, y, x), agg: 2 (over core).
Axes of the slice: x: 2, y: 2, z: 4, core: 2. Of those that a mesh axis runs over, the one named last changes fastest.
Arguments:
- block_values: float32 [7, 4, 4, 32768], P(None, None, None, ('sub', 'agg'))
- block_cols: int32 [7, 32768], P(None, ('sub', 'agg')), may hold values from 0 to 32767, as said below
- coarse_rhs: float32 [4, 32768], P(None, ('sub', 'agg'))
- guess: float32 [4, 32768], P(None, ('sub', 'agg')), may hold values from -3 to 3
- bound_low: int32 [1], replicated, may hold values from 20 to 26
- bound_high: int32 [1], replicated, may hold values from 32 to 40
Outputs:
- smoothed: float32 [4, 32768], P(None, ('sub', 'agg'))
- residual: float32 [4, 32768], P(None, ('sub', 'agg'))
- residual_rms: float32 [1], replicated
The draws below stay inside these ranges and needn't reach their ends.
Inputs may be any that keep to these rules, and one draw needn't show every extreme that they name: Block rows form 32768 / 1024 planes of 1024 consecutive rows, in a periodic order. block_cols[0] is the row itself, block_cols[1] a row of the previous plane, block_cols[2] a row of the next plane, block_cols[3] to block_cols[6] rows of the same plane.
All inputs are finite; a program needn't handle non-finite values.
Results may differ from the reference program's by a relative error of at most 0.0001.
Values sent between devices are 32-bit elements; how exact they have to be, the bound alone decides.
A program may use at most 64 MiB of HBM per device.

```python
import jax
import jax.numpy as jnp
from jax import lax

ROWS_DEV = 1024
COMP = 4
NEIGHBORS = 7
STEPS = 4
TOTAL = 32768


def draw_block_values(key, part):
    noise = 0.5 * jax.random.normal(key, (NEIGHBORS, COMP, COMP, TOTAL), jnp.float32)
    identity = jnp.eye(COMP, dtype=jnp.float32)[:, :, None]
    diagonal_block = noise[0] * (1.0 - identity) + 6.0 * identity
    return jnp.concatenate([diagonal_block[None], noise[1:]], axis=0)


def draw_block_cols(key, part):
    planes = TOTAL // ROWS_DEV
    rows_all = jnp.arange(TOTAL, dtype=jnp.int32)
    plane_of = rows_all // ROWS_DEV
    picked = jax.random.randint(key, (6, TOTAL), 0, ROWS_DEV).astype(jnp.int32)
    before = (plane_of - 1) % planes * ROWS_DEV + picked[0]
    after = (plane_of + 1) % planes * ROWS_DEV + picked[1]
    same_plane = plane_of[None, :] * ROWS_DEV + picked[2:]
    return jnp.concatenate([rows_all[None], before[None], after[None], same_plane], axis=0).astype(jnp.int32)


def draw_coarse_rhs(key, part):
    rows_all = jnp.arange(TOTAL, dtype=jnp.float32)
    scale_row = 0.5 + 0.5 * rows_all / TOTAL
    values = jax.random.normal(key, (COMP, TOTAL), jnp.float32)
    return values * scale_row[None, :]


def steps_of(own_key, extent, cuts, least, high):
    loudness = 1.0
    for dim, shards_of in cuts:
        draws = jax.random.uniform(jax.random.fold_in(jax.random.fold_in(own_key, 6), dim), (shards_of,), jnp.float32, least / len(cuts), high / len(cuts))
        loudness = loudness * jnp.repeat(jnp.exp(draws), extent[dim] // shards_of).reshape((-1,) + (1,) * (len(extent) - 1 - dim))
    return loudness


def scatter_about(rng, shape, scale, limit, cuts=(), held_as=jnp.bfloat16):
    array = jax.random.normal(rng, shape, jnp.float32) * scale
    if len(cuts) > 0:
        array = steps_of(rng, shape, cuts, -0.22, 0.18) * array
    return jnp.clip(array, min=-limit, max=limit).astype(held_as)


def setup_inputs(seed: int = 0) -> dict:
    splits = jax.random.split(jax.random.key(seed), 7)
    block_values = draw_block_values(jax.random.fold_in(splits[6], 71), 0)
    block_cols = draw_block_cols(jax.random.fold_in(splits[6], 71), 0)
    coarse_rhs = draw_coarse_rhs(jax.random.fold_in(splits[6], 71), 0)
    guess = scatter_about(splits[3], (COMP, TOTAL), 0.5, 3.0, ((1, 32),), jnp.float32)
    bound_low = jax.random.randint(splits[4], (1,), 20, 27).astype(jnp.int32)
    bound_high = jax.random.randint(splits[5], (1,), 32, 41).astype(jnp.int32)
    return dict(block_values=block_values, block_cols=block_cols, coarse_rhs=coarse_rhs, guess=guess, bound_low=bound_low, bound_high=bound_high)


def apply_blocks(block_values, position, field):
    count = position.shape[0]
    width = position.shape[1]
    taken = jnp.take(field, position.reshape(-1), axis=1).reshape(field.shape[0], count, width)
    result = jnp.zeros((field.shape[0], width), jnp.float32)
    for column in range(field.shape[0]):
        result = result + lax.optimization_barrier(jnp.sum(block_values[:, :, column, :] * taken[column][:, None, :], axis=0))
    return result

def reference(block_values, block_cols, coarse_rhs, guess, bound_low, bound_high):
    lower = bound_low[0].astype(jnp.float32) / 4.0
    upper = bound_high[0].astype(jnp.float32) / 4.0
    centre = (upper + lower) / 2.0
    half_width = (upper - lower) / 2.0
    spread_ratio = centre / half_width
    ratio_prev = 1.0 / spread_ratio
    smoothed = guess
    residual = coarse_rhs - apply_blocks(block_values, block_cols, guess)
    direction = residual / centre
    for step in range(STEPS):
        smoothed = smoothed + direction
        residual = residual - apply_blocks(block_values, block_cols, direction)
        if step + 1 < STEPS:
            ratio_next = 1.0 / (2.0 * spread_ratio - ratio_prev)
            direction = ratio_next * ratio_prev * direction + 2.0 * ratio_next / half_width * residual
            ratio_prev = ratio_next
    total_sq = jnp.sum(residual * residual)
    residual_rms = jnp.sqrt(total_sq / (4.0 * TOTAL) + 1e-06).reshape(1)
    return (smoothed, residual, residual_rms)
```

```python
import functools

import jax
import jax.numpy as jnp
from jax import lax
from jax.experimental import pallas as pl
from jax.experimental.pallas import tpu as pltpu
from jax.sharding import PartitionSpec as P

STEPS = 4
ONE_ROUND = 32
LANES = 128
MESH = pl.DeviceIdType.MESH


def gather_lanes(rows, index):
    return jnp.take_along_axis(rows, index, axis=1, mode="promise_in_bounds")


def kernel(
    subs, aggs, shape,
    values_hbm, cols_hbm, rhs_hbm, guess_hbm, low_ref, high_ref,
    smoothed_out, residual_out, rms_ref,
    values, cols, cols_flat, rhs, field, beside, lane_of, tile_of, coef,
    near_sums, far_sums,
    values_sem, load_sem, send_sem, recv_sem,
    near_send, near_recv, far_send, far_recv,
):
    blocks, comp, tiles = shape
    devices = subs * aggs
    rows = tiles * LANES
    load_cols = pltpu.make_async_copy(cols_hbm, cols, load_sem.at[0])
    load_guess = pltpu.make_async_copy(guess_hbm, field.at[0], load_sem.at[1])
    load_rhs = pltpu.make_async_copy(rhs_hbm, rhs, load_sem.at[2])
    for load in (load_guess, load_cols):
        load.start()
    own = [0] + list(range(3, blocks))
    per_block = comp * comp * tiles

    def load_values(k):
        part = pl.ds(k * per_block, per_block)
        return pltpu.make_async_copy(values_hbm.at[part], values.at[part], values_sem.at[k])

    for k in own + [1, 2]:
        load_values(k).start()
    load_rhs.start()

    sub, agg = lax.axis_index("sub"), lax.axis_index("agg")
    me = sub * aggs + agg

    def ahead_of(place, by, size):
        to = place + by
        return jnp.where(to >= size, to - size, to)

    def beside_me(by_sub, by_agg):
        return (ahead_of(sub, by_sub, subs), ahead_of(agg, by_agg, aggs))

    def ring(way):
        turn = jnp.where(way == 0, agg == aggs - 1, agg == 0)
        to_sub = jnp.where(way == 0, ahead_of(sub, 1, subs), ahead_of(sub, subs - 1, subs))
        to_agg = jnp.where(way == 0, ahead_of(agg, 1, aggs), ahead_of(agg, aggs - 1, aggs))
        return (jnp.where(turn, to_sub, sub), to_agg)

    following = ahead_of(me, 1, devices)
    previous = ahead_of(me, devices - 1, devices)
    one_round = devices <= ONE_ROUND
    if one_round:
        near_steps = [(a, b) for a in range(subs) for b in range(aggs)][1:]
        near_steps = near_steps[::-1]
        near, near_me = devices, me
        far_steps = []
    else:
        near_steps = [(0, b) for b in range(1, aggs)]
        near, near_me = aggs, agg
        far_steps = [(a, 0) for a in range(1, subs)]
    near_partners = [beside_me(a, b) for a, b in near_steps]
    far_partners = [beside_me(a, b) for a, b in far_steps]

    barrier = pltpu.get_barrier_semaphore()
    partners = far_partners + near_partners
    if not one_round:
        partners = [ring(0), ring(1)] + partners
    for partner in partners:
        pl.semaphore_signal(barrier, inc=1, device_id=partner, device_id_type=MESH)

    load_guess.wait()
    pl.semaphore_wait(barrier, len(partners))

    def send(step, source, way):
        return pltpu.make_async_remote_copy(
            src_ref=source,
            dst_ref=beside.at[step, way],
            send_sem=send_sem.at[step, way],
            recv_sem=recv_sem.at[step, way],
            device_id=ring(way),
            device_id_type=MESH,
        )

    for way in range(2):
        send(0, field.at[0], way).start()

    low = jnp.full((tiles, LANES), low_ref[0], jnp.int32).astype(jnp.float32) / 4.0
    high = jnp.full((tiles, LANES), high_ref[0], jnp.int32).astype(jnp.float32) / 4.0
    centre = (high + low) / 2.0
    half = (high - low) / 2.0
    spread = centre / half
    ratio = 1.0 / spread
    coef[0, 0] = jnp.zeros((tiles, LANES), jnp.float32)
    coef[0, 1] = 1.0 / centre
    for t in range(1, STEPS):
        ahead = 1.0 / (2.0 * spread - ratio)
        coef[t, 0] = ahead * ratio
        coef[t, 1] = 2.0 * ahead / half
        ratio = ahead

    load_cols.wait()
    for c in range(tiles):
        cols_flat[pl.ds(c * 8, blocks), :] = cols[:, c * LANES:(c + 1) * LANES]
    for k in range(1, blocks):
        plane = {1: previous, 2: following}.get(k, me)
        local = cols_flat[pl.ds(k, tiles, stride=8), :] - plane * rows
        lane_of[k] = local & (LANES - 1)
        tile_of[k] = local >> 7

    def taken(source, k):
        lanes, tile = lane_of[k], tile_of[k]
        out = [None] * comp
        for r in range(tiles):
            here = tile == r
            for j in range(comp):
                row = jnp.broadcast_to(source[pl.ds(r * comp + j, 1), :], (tiles, LANES))
                got = gather_lanes(row, lanes)
                out[j] = got if r == 0 else jnp.where(here, got, out[j])
        return out

    def combine(k, got, total):
        total = list(total)
        for i in range(comp):
            base = (k * comp + i) * comp * tiles
            for j in range(comp):
                total[i] = total[i] - values[pl.ds(base + j, tiles, stride=comp), :] * got[j]
        return total

    def own_part(t, residual):
        source = field.at[t]
        direct = [source[pl.ds(j, tiles, stride=comp), :] for j in range(comp)]
        residual = combine(0, direct, residual)
        for k in own[1:]:
            residual = combine(k, taken(source, k), residual)
        return direct, residual

    def far_part(t, residual):
        even = 1 - lax.rem(me, 2)
        for way in (even, 1 - even):
            send(t, field.at[t], way).wait_recv()
            residual = combine(1 + way, taken(beside.at[t, way], 1 + way), residual)
        return residual

    load_rhs.wait()
    for k in own + [1, 2]:
        load_values(k).wait()

    def step(t, carry):
        smoothed, residual = carry
        direct, residual = own_part(t, residual)
        smoothed = [s + d for s, d in zip(smoothed, direct)]
        residual = far_part(t, residual)
        for j in range(comp):
            field[t + 1, pl.ds(j, tiles, stride=comp), :] = (
                coef[t, 0] * direct[j] + coef[t, 1] * residual[j]
            )
        for way in range(2):
            send(t + 1, field.at[t + 1], way).start()
        return smoothed, residual

    smoothed = [jnp.zeros((tiles, LANES), jnp.float32) for j in range(comp)]
    residual = [rhs[pl.ds(j, tiles, stride=comp), :] for j in range(comp)]
    smoothed, residual = lax.fori_loop(0, STEPS, step, (smoothed, residual))

    direct, residual = own_part(STEPS, residual)
    for j in range(comp):
        smoothed_out[pl.ds(j, tiles, stride=comp), :] = smoothed[j] + direct[j]
    residual = far_part(STEPS, residual)

    squares = residual[0] * residual[0]
    for j in range(1, comp):
        squares = squares + residual[j] * residual[j]
    partial = jnp.sum(squares, axis=0, keepdims=True)

    def spread_sums(sums, slot, partner, send_sems, recv_sems, d):
        return pltpu.make_async_remote_copy(
            src_ref=sums.at[slot],
            dst_ref=sums.at[slot],
            send_sem=send_sems.at[d],
            recv_sem=recv_sems.at[slot],
            device_id=partner,
            device_id_type=MESH,
        )

    def slot_of(partner):
        return partner[0] * aggs + partner[1] if one_round else partner[1]

    near_sums[near_me] = partial
    for d, partner in enumerate(near_partners):
        spread_sums(near_sums, near_me, partner, near_send, near_recv, d).start()
    for j in range(comp):
        residual_out[pl.ds(j, tiles, stride=comp), :] = residual[j]
    for d, partner in enumerate(near_partners):
        spread_sums(near_sums, slot_of(partner), partner, near_send, near_recv, d).wait_recv()
    total = jnp.sum(near_sums[...], axis=0)
    if far_partners:
        far_sums[sub] = total
        for d, partner in enumerate(far_partners):
            spread_sums(far_sums, sub, partner, far_send, far_recv, d).start()
        for d, partner in enumerate(far_partners):
            spread_sums(far_sums, partner[0], partner, far_send, far_recv, d).wait_recv()
        total = jnp.sum(far_sums[...], axis=0)
    count = float(comp * rows * devices)
    rms_ref[...] = jnp.broadcast_to(jnp.sqrt(jnp.sum(total, axis=1, keepdims=True) / count + 1e-06), rms_ref.shape)

    for t in range(STEPS + 1):
        for way in range(2):
            send(t, field.at[t], way).wait_send()
    for d, partner in enumerate(near_partners):
        spread_sums(near_sums, near_me, partner, near_send, near_recv, d).wait_send()
    for d, partner in enumerate(far_partners):
        spread_sums(far_sums, sub, partner, far_send, far_recv, d).wait_send()


def put_out(*refs):
    count = len(refs) // 2
    sems = refs[-1]
    copies = [
        pltpu.make_async_copy(refs[i] if i < 2 else refs[i].at[pl.ds(0, 1)], refs[count + i], sems.at[i]) for i in range(count)
    ]
    for copy in copies:
        copy.start()
    for copy in copies:
        copy.wait()


def flat(field, tiles):
    comp = field.shape[-2]
    lead = field.shape[:-2]
    cut = field.reshape(lead + (comp, tiles, LANES))
    return jnp.swapaxes(cut, -3, -2).reshape(-1, LANES)


def unflat(field, comp):
    tiles = field.shape[0] // comp
    return jnp.swapaxes(field.reshape(tiles, comp, LANES), 0, 1).reshape(comp, tiles * LANES)


def shards(subs, aggs, block_values, block_cols, coarse_rhs, guess, bound_low, bound_high):
    blocks, comp, _, rows = block_values.shape
    tiles = rows // LANES
    devices = subs * aggs
    near, far = (devices, 1) if devices <= ONE_ROUND else (aggs, subs)
    f32 = jnp.float32
    plane = (tiles * comp, LANES)
    anywhere = pl.BlockSpec(memory_space=pl.ANY)
    in_vmem = pl.BlockSpec(memory_space=pltpu.VMEM)
    in_hbm = pl.BlockSpec(memory_space=pltpu.HBM)
    dma = pltpu.SemaphoreType.DMA
    smoothed, residual, rms = pl.pallas_call(
        functools.partial(kernel, subs, aggs, (blocks, comp, tiles)),
        out_shape=(
            jax.ShapeDtypeStruct(plane, f32),
            jax.ShapeDtypeStruct(plane, f32),
            jax.ShapeDtypeStruct((8, LANES), f32),
        ),
        in_specs=[in_hbm] * 4 + [pl.BlockSpec(memory_space=pltpu.SMEM)] * 2,
        out_specs=(in_vmem,) * 3,
        scratch_shapes=[
            pltpu.VMEM((blocks * comp * comp * tiles, LANES), f32),
            pltpu.VMEM((blocks, rows), jnp.int32),
            pltpu.VMEM((8 * tiles, LANES), jnp.int32),
            pltpu.VMEM(plane, f32),
            pltpu.VMEM((STEPS + 1,) + plane, f32),
            pltpu.VMEM((STEPS + 1, 2) + plane, f32),
            pltpu.VMEM((blocks, tiles, LANES), jnp.int32),
            pltpu.VMEM((blocks, tiles, LANES), jnp.int32),
            pltpu.VMEM((STEPS, 2, tiles, LANES), f32),
            pltpu.VMEM((near, 1, LANES), f32),
            pltpu.VMEM((far, 1, LANES), f32),
            dma((blocks,)),
            dma((5,)),
            dma((STEPS + 1, 2)),
            dma((STEPS + 1, 2)),
            dma((max(near - 1, 1),)),
            dma((near,)),
            dma((max(far - 1, 1),)),
            dma((far,)),
        ],
        compiler_params=pltpu.CompilerParams(collective_id=0, has_side_effects=True, vmem_limit_bytes=8 * 1024 * 1024),
    )(
        *[
            pltpu.with_memory_space_constraint(x, pltpu.HBM)
            for x in (
                flat(block_values, tiles), block_cols, flat(coarse_rhs, tiles), flat(guess, tiles),
            )
        ],
        bound_low, bound_high,
    )
    smoothed, residual, rms = pl.pallas_call(
        put_out,
        out_shape=(
            jax.ShapeDtypeStruct(plane, f32),
            jax.ShapeDtypeStruct(plane, f32),
            jax.ShapeDtypeStruct((1, LANES), f32),
        ),
        in_specs=[anywhere] * 3,
        out_specs=(anywhere,) * 3,
        scratch_shapes=[dma((3,))],
        compiler_params=pltpu.CompilerParams(vmem_limit_bytes=8 * 1024 * 1024),
    )(smoothed, residual, rms)
    return unflat(smoothed, comp), unflat(residual, comp), rms[0,:1]


def solution(mesh):
    split = ("sub", "agg")
    return jax.shard_map(
        functools.partial(shards, mesh.shape["sub"], mesh.shape["agg"]),
        mesh=mesh,
        in_specs=(
            P(None, None, None, split),
            P(None, split),
            P(None, split),
            P(None, split),
            P(),
            P(),
        ),
        out_specs=(P(None, split), P(None, split), P()),
        check_vma=False,
    )
```

```python
import functools

import jax
import jax.numpy as jnp
from jax import lax
from jax.experimental import pallas as pl
from jax.experimental.pallas import tpu as pltpu
from jax.sharding import PartitionSpec as P

STEPS = 4
ONE_ROUND = 32
GHOSTS = 1
LANES = 128
MESH = pl.DeviceIdType.MESH


def gather_lanes(rows, index):
    return jnp.take_along_axis(rows, index, axis=1, mode="promise_in_bounds")


def kernel(
    subs, aggs, shape,
    values_hbm, cols_hbm, rhs_hbm, guess_hbm, low_ref, high_ref,
    smoothed_out, residual_out, rms_ref,
    values, cols, cols_flat, rhs, field, beside, lane_of, tile_of, coef,
    near_sums, far_sums,
    ghost_values, ghost_cols, ghost_flat, ghost_lane, ghost_tile, ghost_residual, beyond,
    values_sem, load_sem, send_sem, recv_sem,
    near_send, near_recv, far_send, far_recv,
    ghost_send, ghost_recv, beyond_send, beyond_recv,
):
    blocks, comp, tiles = shape
    devices = subs * aggs
    rows = tiles * LANES
    load_cols = pltpu.make_async_copy(cols_hbm, cols, load_sem.at[0])
    load_guess = pltpu.make_async_copy(guess_hbm, field.at[0], load_sem.at[1])
    load_rhs = pltpu.make_async_copy(rhs_hbm, rhs, load_sem.at[2])
    for load in (load_guess, load_cols):
        load.start()
    own = [0] + list(range(3, blocks))
    per_block = comp * comp * tiles

    def load_values(k):
        part = pl.ds(k * per_block, per_block)
        return pltpu.make_async_copy(values_hbm.at[part], values.at[part], values_sem.at[k])

    for k in own + [1, 2]:
        load_values(k).start()
    load_rhs.start()

    sub, agg = lax.axis_index("sub"), lax.axis_index("agg")
    me = sub * aggs + agg

    def ahead_of(place, by, size):
        to = place + by
        return jnp.where(to >= size, to - size, to)

    def beside_me(by_sub, by_agg):
        return (ahead_of(sub, by_sub, subs), ahead_of(agg, by_agg, aggs))

    def ring(way):
        turn = jnp.where(way == 0, agg == aggs - 1, agg == 0)
        to_sub = jnp.where(way == 0, ahead_of(sub, 1, subs), ahead_of(sub, subs - 1, subs))
        to_agg = jnp.where(way == 0, ahead_of(agg, 1, aggs), ahead_of(agg, aggs - 1, aggs))
        return (jnp.where(turn, to_sub, sub), to_agg)

    following = ahead_of(me, 1, devices)
    previous = ahead_of(me, devices - 1, devices)
    one_round = devices <= ONE_ROUND
    if one_round:
        near_steps = [(a, b) for a in range(subs) for b in range(aggs)][1:]
        near_steps = near_steps[::-1]
        near, near_me = devices, me
        far_steps = []
    else:
        near_steps = [(0, b) for b in range(1, aggs)]
        near, near_me = aggs, agg
        far_steps = [(a, 0) for a in range(1, subs)]
    near_partners = [beside_me(a, b) for a, b in near_steps]
    far_partners = [beside_me(a, b) for a, b in far_steps]

    ghosts = GHOSTS if one_round and devices % (2 * GHOSTS) == 0 else 0
    even = 1 - lax.rem(me, 2)
    across = 1 - even

    def has_ghost(border):
        return lax.rem(border + 1, devices // ghosts) == 0

    if ghosts:
        inner = jnp.where(even == 1, following, previous)
        outer = jnp.where(even == 1, previous, following)
        own_ghost = has_ghost(jnp.where(even == 1, previous, me))
        feeds = has_ghost(jnp.where(even == 1, following, ahead_of(me, devices - 2, devices)))
        second = jnp.where(even == 1, ahead_of(me, 2, devices), ahead_of(me, devices - 2, devices))
        fed = (second // aggs, lax.rem(second, aggs))

    barrier = pltpu.get_barrier_semaphore()
    partners = far_partners + near_partners
    if not one_round:
        partners = [ring(0), ring(1)] + partners
    for partner in partners:
        pl.semaphore_signal(barrier, inc=1, device_id=partner, device_id_type=MESH)

    load_guess.wait()
    pl.semaphore_wait(barrier, len(partners))

    def send(step, source, way):
        return pltpu.make_async_remote_copy(
            src_ref=source,
            dst_ref=beside.at[step, way],
            send_sem=send_sem.at[step, way],
            recv_sem=recv_sem.at[step, way],
            device_id=ring(way),
            device_id_type=MESH,
        )

    for way in range(2):
        send(0, field.at[0], way).start()

    def feed(t):
        return pltpu.make_async_remote_copy(
            src_ref=field.at[t],
            dst_ref=beyond.at[t],
            send_sem=beyond_send.at[t],
            recv_sem=beyond_recv.at[t],
            device_id=fed,
            device_id_type=MESH,
        )

    def give(k):
        source, target = cols, ghost_cols
        if k < blocks:
            part = pl.ds(k * per_block, per_block)
            source, target = values.at[part], ghost_values.at[part]
        return pltpu.make_async_remote_copy(
            src_ref=source,
            dst_ref=target,
            send_sem=ghost_send.at[k],
            recv_sem=ghost_recv.at[k],
            device_id=ring(even),
            device_id_type=MESH,
        )

    def crosses(t, way):
        if not ghosts:
            return True
        return jnp.logical_not(own_ghost & (way == across) & (t >= 2))

    low = jnp.full((tiles, LANES), low_ref[0], jnp.int32).astype(jnp.float32) / 4.0
    high = jnp.full((tiles, LANES), high_ref[0], jnp.int32).astype(jnp.float32) / 4.0
    centre = (high + low) / 2.0
    half = (high - low) / 2.0
    spread = centre / half
    ratio = 1.0 / spread
    coef[0, 0] = jnp.zeros((tiles, LANES), jnp.float32)
    coef[0, 1] = 1.0 / centre
    for t in range(1, STEPS):
        ahead = 1.0 / (2.0 * spread - ratio)
        coef[t, 0] = ahead * ratio
        coef[t, 1] = 2.0 * ahead / half
        ratio = ahead

    def index(cols, cols_flat, lane_of, tile_of, before, here, after):
        for c in range(tiles):
            cols_flat[pl.ds(c * 8, blocks), :] = cols[:, c * LANES:(c + 1) * LANES]
        for k in range(1, blocks):
            plane = {1: before, 2: after}.get(k, here)
            local = cols_flat[pl.ds(k, tiles, stride=8), :] - plane * rows
            lane_of[k] = local & (LANES - 1)
            tile_of[k] = local >> 7

    load_cols.wait()
    index(cols, cols_flat, lane_of, tile_of, previous, me, following)

    def taken(source, k, lane_of=lane_of, tile_of=tile_of):
        lanes, tile = lane_of[k], tile_of[k]
        out = [None] * comp
        for r in range(tiles):
            here = tile == r
            for j in range(comp):
                row = jnp.broadcast_to(source[pl.ds(r * comp + j, 1), :], (tiles, LANES))
                got = gather_lanes(row, lanes)
                out[j] = got if r == 0 else jnp.where(here, got, out[j])
        return out

    def combine(k, got, total, values=values):
        total = list(total)
        for i in range(comp):
            base = (k * comp + i) * comp * tiles
            for j in range(comp):
                total[i] = total[i] - values[pl.ds(base + j, tiles, stride=comp), :] * got[j]
        return total

    def own_part(t, residual):
        source = field.at[t]
        direct = [source[pl.ds(j, tiles, stride=comp), :] for j in range(comp)]
        residual = combine(0, direct, residual)
        for k in own[1:]:
            residual = combine(k, taken(source, k), residual)
        return direct, residual

    def far_part(t, residual):
        for way in (even, across):
            @pl.when(crosses(t, way))
            def _():
                send(t, field.at[t], way).wait_recv()
            residual = combine(1 + way, taken(beside.at[t, way], 1 + way), residual)
        return residual

    load_rhs.wait()
    for k in own + [1, 2]:
        load_values(k).wait()

    if ghosts:
        ghost_residual[...] = jnp.zeros(ghost_residual.shape, jnp.float32)

        @pl.when(own_ghost)
        def _():
            for k in [blocks] + own + [1, 2]:
                give(k).start()

    def ghost_step(t):
        @pl.when(t == 1)
        def _():
            for k in [blocks] + own + [1, 2]:
                give(k).wait_recv()
            here, past = outer, jnp.where(even == 1, ahead_of(me, devices - 2, devices), ahead_of(me, 2, devices))
            before = jnp.where(even == 1, past, me)
            after = jnp.where(even == 1, me, past)
            index(ghost_cols, ghost_flat, ghost_lane, ghost_tile, before, here, after)
            for j in range(comp):
                ghost_residual[j] = centre * beside[1, across, pl.ds(j, tiles, stride=comp), :]

        source = beside.at[t, across]
        direct = [source[pl.ds(j, tiles, stride=comp), :] for j in range(comp)]
        total = [ghost_residual[j] for j in range(comp)]
        total = combine(0, direct, total, ghost_values)
        for k in own[1:]:
            total = combine(k, taken(source, k, ghost_lane, ghost_tile), total, ghost_values)
        k = 2 - across
        total = combine(k, taken(field.at[t], k, ghost_lane, ghost_tile), total, ghost_values)
        feed(t).wait_recv()
        k = 1 + across
        total = combine(k, taken(beyond.at[t], k, ghost_lane, ghost_tile), total, ghost_values)
        for j in range(comp):
            ghost_residual[j] = total[j]
            beside[t + 1, across, pl.ds(j, tiles, stride=comp), :] = (
                coef[t, 0] * direct[j] + coef[t, 1] * total[j]
            )

    def step(t, carry):
        smoothed, residual = carry
        direct, residual = own_part(t, residual)
        smoothed = [s + d for s, d in zip(smoothed, direct)]
        residual = far_part(t, residual)
        for j in range(comp):
            field[t + 1, pl.ds(j, tiles, stride=comp), :] = (
                coef[t, 0] * direct[j] + coef[t, 1] * residual[j]
            )
        for way in range(2):
            @pl.when(crosses(t + 1, 1 - way))
            def _():
                send(t + 1, field.at[t + 1], way).start()
        if ghosts:
            @pl.when(feeds & (t + 1 < STEPS))
            def _():
                feed(t + 1).start()

            @pl.when(own_ghost & (t >= 1) & (t < STEPS))
            def _():
                ghost_step(t)
        return smoothed, residual

    smoothed = [jnp.zeros((tiles, LANES), jnp.float32) for j in range(comp)]
    residual = [rhs[pl.ds(j, tiles, stride=comp), :] for j in range(comp)]
    smoothed, residual = lax.fori_loop(0, STEPS, step, (smoothed, residual))

    direct, residual = own_part(STEPS, residual)
    for j in range(comp):
        smoothed_out[pl.ds(j, tiles, stride=comp), :] = smoothed[j] + direct[j]
    residual = far_part(STEPS, residual)

    squares = residual[0] * residual[0]
    for j in range(1, comp):
        squares = squares + residual[j] * residual[j]
    partial = jnp.sum(squares, axis=0, keepdims=True)

    def spread_sums(sums, slot, partner, send_sems, recv_sems, d):
        return pltpu.make_async_remote_copy(
            src_ref=sums.at[slot],
            dst_ref=sums.at[slot],
            send_sem=send_sems.at[d],
            recv_sem=recv_sems.at[slot],
            device_id=partner,
            device_id_type=MESH,
        )

    def slot_of(partner):
        return partner[0] * aggs + partner[1] if one_round else partner[1]

    near_sums[near_me] = partial
    for d, partner in enumerate(near_partners):
        spread_sums(near_sums, near_me, partner, near_send, near_recv, d).start()
    for j in range(comp):
        residual_out[pl.ds(j, tiles, stride=comp), :] = residual[j]
    for d, partner in enumerate(near_partners):
        spread_sums(near_sums, slot_of(partner), partner, near_send, near_recv, d).wait_recv()
    total = jnp.sum(near_sums[...], axis=0)
    if far_partners:
        far_sums[sub] = total
        for d, partner in enumerate(far_partners):
            spread_sums(far_sums, sub, partner, far_send, far_recv, d).start()
        for d, partner in enumerate(far_partners):
            spread_sums(far_sums, partner[0], partner, far_send, far_recv, d).wait_recv()
        total = jnp.sum(far_sums[...], axis=0)
    count = float(comp * rows * devices)
    rms_ref[...] = jnp.broadcast_to(jnp.sqrt(jnp.sum(total, axis=1, keepdims=True) / count + 1e-06), rms_ref.shape)

    for t in range(STEPS + 1):
        for way in range(2):
            @pl.when(crosses(t, 1 - way))
            def _():
                send(t, field.at[t], way).wait_send()
    if ghosts:
        @pl.when(feeds)
        def _():
            for t in range(1, STEPS):
                feed(t).wait_send()

        @pl.when(own_ghost)
        def _():
            for k in range(blocks + 1):
                give(k).wait_send()
    for d, partner in enumerate(near_partners):
        spread_sums(near_sums, near_me, partner, near_send, near_recv, d).wait_send()
    for d, partner in enumerate(far_partners):
        spread_sums(far_sums, sub, partner, far_send, far_recv, d).wait_send()


def put_out(*refs):
    count = len(refs) // 2
    sems = refs[-1]
    copies = [
        pltpu.make_async_copy(refs[i] if i < 2 else refs[i].at[pl.ds(0, 1)], refs[count + i], sems.at[i]) for i in range(count)
    ]
    for copy in copies:
        copy.start()
    for copy in copies:
        copy.wait()


def flat(field, tiles):
    comp = field.shape[-2]
    lead = field.shape[:-2]
    cut = field.reshape(lead + (comp, tiles, LANES))
    return jnp.swapaxes(cut, -3, -2).reshape(-1, LANES)


def unflat(field, comp):
    tiles = field.shape[0] // comp
    return jnp.swapaxes(field.reshape(tiles, comp, LANES), 0, 1).reshape(comp, tiles * LANES)


def shards(subs, aggs, block_values, block_cols, coarse_rhs, guess, bound_low, bound_high):
    blocks, comp, _, rows = block_values.shape
    tiles = rows // LANES
    devices = subs * aggs
    near, far = (devices, 1) if devices <= ONE_ROUND else (aggs, subs)
    f32 = jnp.float32
    plane = (tiles * comp, LANES)
    anywhere = pl.BlockSpec(memory_space=pl.ANY)
    in_vmem = pl.BlockSpec(memory_space=pltpu.VMEM)
    in_hbm = pl.BlockSpec(memory_space=pltpu.HBM)
    dma = pltpu.SemaphoreType.DMA
    smoothed, residual, rms = pl.pallas_call(
        functools.partial(kernel, subs, aggs, (blocks, comp, tiles)),
        out_shape=(
            jax.ShapeDtypeStruct(plane, f32),
            jax.ShapeDtypeStruct(plane, f32),
            jax.ShapeDtypeStruct((8, LANES), f32),
        ),
        in_specs=[in_hbm] * 4 + [pl.BlockSpec(memory_space=pltpu.SMEM)] * 2,
        out_specs=(in_vmem,) * 3,
        scratch_shapes=[
            pltpu.VMEM((blocks * comp * comp * tiles, LANES), f32),
            pltpu.VMEM((blocks, rows), jnp.int32),
            pltpu.VMEM((8 * tiles, LANES), jnp.int32),
            pltpu.VMEM(plane, f32),
            pltpu.VMEM((STEPS + 1,) + plane, f32),
            pltpu.VMEM((STEPS + 1, 2) + plane, f32),
            pltpu.VMEM((blocks, tiles, LANES), jnp.int32),
            pltpu.VMEM((blocks, tiles, LANES), jnp.int32),
            pltpu.VMEM((STEPS, 2, tiles, LANES), f32),
            pltpu.VMEM((near, 1, LANES), f32),
            pltpu.VMEM((far, 1, LANES), f32),
            pltpu.VMEM((blocks * comp * comp * tiles, LANES), f32),
            pltpu.VMEM((blocks, rows), jnp.int32),
            pltpu.VMEM((8 * tiles, LANES), jnp.int32),
            pltpu.VMEM((blocks, tiles, LANES), jnp.int32),
            pltpu.VMEM((blocks, tiles, LANES), jnp.int32),
            pltpu.VMEM((comp, tiles, LANES), f32),
            pltpu.VMEM((STEPS + 1,) + plane, f32),
            dma((blocks,)),
            dma((5,)),
            dma((STEPS + 1, 2)),
            dma((STEPS + 1, 2)),
            dma((max(near - 1, 1),)),
            dma((near,)),
            dma((max(far - 1, 1),)),
            dma((far,)),
            dma((blocks + 1,)),
            dma((blocks + 1,)),
            dma((STEPS + 1,)),
            dma((STEPS + 1,)),
        ],
        compiler_params=pltpu.CompilerParams(collective_id=0, has_side_effects=True, vmem_limit_bytes=8 * 1024 * 1024),
    )(
        *[
            pltpu.with_memory_space_constraint(x, pltpu.HBM)
            for x in (
                flat(block_values, tiles), block_cols, flat(coarse_rhs, tiles), flat(guess, tiles),
            )
        ],
        bound_low, bound_high,
    )
    smoothed, residual, rms = pl.pallas_call(
        put_out,
        out_shape=(
            jax.ShapeDtypeStruct(plane, f32),
            jax.ShapeDtypeStruct(plane, f32),
            jax.ShapeDtypeStruct((1, LANES), f32),
        ),
        in_specs=[anywhere] * 3,
        out_specs=(anywhere,) * 3,
        scratch_shapes=[dma((3,))],
        compiler_params=pltpu.CompilerParams(vmem_limit_bytes=8 * 1024 * 1024),
    )(smoothed, residual, rms)
    return unflat(smoothed, comp), unflat(residual, comp), rms[0,:1]


def solution(mesh):
    split = ("sub", "agg")
    return jax.shard_map(
        functools.partial(shards, mesh.shape["sub"], mesh.shape["agg"]),
        mesh=mesh,
        in_specs=(
            P(None, None, None, split),
            P(None, split),
            P(None, split),
            P(None, split),
            P(),
            P(),
        ),
        out_specs=(P(None, split), P(None, split), P()),
        check_vma=False,
    )
```

```python
import functools

import jax
import jax.numpy as jnp
from jax import lax
from jax.experimental import pallas as pl
from jax.experimental.pallas import tpu as pltpu
from jax.sharding import PartitionSpec as P

STEPS = 4
ONE_ROUND = 32
GHOSTS = 4
FIRST_EVEN = 3
FIRST_ODD = 8
LANES = 128
MESH = pl.DeviceIdType.MESH


def gather_lanes(rows, index):
    return jnp.take_along_axis(rows, index, axis=1, mode="promise_in_bounds")


def kernel(
    subs, aggs, shape,
    values_hbm, cols_hbm, rhs_hbm, guess_hbm, low_ref, high_ref,
    smoothed_out, residual_out, rms_ref,
    values, cols, cols_flat, rhs, field, beside, lane_of, tile_of, coef,
    near_sums, far_sums,
    ghost_values, ghost_cols, ghost_flat, ghost_lane, ghost_tile, ghost_residual, beyond,
    values_sem, load_sem, send_sem, recv_sem,
    near_sems, far_sems,
    ghost_send, ghost_recv, beyond_send, beyond_recv,
):
    blocks, comp, tiles = shape
    devices = subs * aggs
    rows = tiles * LANES
    load_cols = pltpu.make_async_copy(cols_hbm, cols, load_sem.at[0])
    load_guess = pltpu.make_async_copy(guess_hbm, field.at[0], load_sem.at[1])
    load_rhs = pltpu.make_async_copy(rhs_hbm, rhs, load_sem.at[2])
    for load in (load_guess, load_cols):
        load.start()
    own = [0] + list(range(3, blocks))
    per_block = comp * comp * tiles

    def load_values(k):
        part = pl.ds(k * per_block, per_block)
        return pltpu.make_async_copy(values_hbm.at[part], values.at[part], values_sem.at[k])

    for k in own + [1, 2]:
        load_values(k).start()
    load_rhs.start()

    sub, agg = lax.axis_index("sub"), lax.axis_index("agg")
    me = sub * aggs + agg

    def ahead_of(place, by, size):
        to = place + by
        return jnp.where(to >= size, to - size, to)

    def beside_me(by_sub, by_agg):
        return (ahead_of(sub, by_sub, subs), ahead_of(agg, by_agg, aggs))

    def ring(way):
        turn = jnp.where(way == 0, agg == aggs - 1, agg == 0)
        to_sub = jnp.where(way == 0, ahead_of(sub, 1, subs), ahead_of(sub, subs - 1, subs))
        to_agg = jnp.where(way == 0, ahead_of(agg, 1, aggs), ahead_of(agg, aggs - 1, aggs))
        return (jnp.where(turn, to_sub, sub), to_agg)

    following = ahead_of(me, 1, devices)
    previous = ahead_of(me, devices - 1, devices)
    one_round = devices <= ONE_ROUND
    if one_round:
        near_steps = [(a, b) for a in range(subs) for b in range(aggs)][1:]
        near_steps.sort(key=lambda step: min(step[0], subs - step[0]))
        near, near_me = devices, me
        far_steps = []
    else:
        near_steps = [(0, b) for b in range(1, aggs)]
        near, near_me = aggs, agg
        far_steps = [(a, 0) for a in range(1, subs)]
    near_partners = [beside_me(a, b) for a, b in near_steps]
    far_partners = [beside_me(a, b) for a, b in far_steps]

    ghosts = GHOSTS if one_round and devices % (2 * GHOSTS) == 0 else 0
    even = 1 - lax.rem(me, 2)
    across = 1 - even

    def has_ghost(border):
        return lax.rem(border + 1, devices // ghosts) == 0

    if ghosts:
        inner = jnp.where(even == 1, following, previous)
        outer = jnp.where(even == 1, previous, following)
        own_ghost = has_ghost(jnp.where(even == 1, previous, me))
        feeds = has_ghost(jnp.where(even == 1, following, ahead_of(me, devices - 2, devices)))
        second = jnp.where(even == 1, ahead_of(me, 2, devices), ahead_of(me, devices - 2, devices))
        fed = (second // aggs, lax.rem(second, aggs))

    barrier = pltpu.get_barrier_semaphore()
    partners = far_partners + near_partners
    if not one_round:
        partners = [ring(0), ring(1)] + partners
    for partner in partners:
        pl.semaphore_signal(barrier, inc=1, device_id=partner, device_id_type=MESH)

    load_guess.wait()
    pl.semaphore_wait(barrier, len(partners))

    def send(step, source, way):
        return pltpu.make_async_remote_copy(
            src_ref=source,
            dst_ref=beside.at[step, way],
            send_sem=send_sem.at[step, way],
            recv_sem=recv_sem.at[step, way],
            device_id=ring(way),
            device_id_type=MESH,
        )

    for way in range(2):
        send(0, field.at[0], way).start()

    def feed(t):
        return pltpu.make_async_remote_copy(
            src_ref=field.at[t],
            dst_ref=beyond.at[t],
            send_sem=beyond_send.at[t],
            recv_sem=beyond_recv.at[t],
            device_id=fed,
            device_id_type=MESH,
        )

    def give(k):
        source, target = cols, ghost_cols
        if k < blocks:
            part = pl.ds(k * per_block, per_block)
            source, target = values.at[part], ghost_values.at[part]
        return pltpu.make_async_remote_copy(
            src_ref=source,
            dst_ref=target,
            send_sem=ghost_send.at[k],
            recv_sem=ghost_recv.at[k],
            device_id=ring(even),
            device_id_type=MESH,
        )

    given = own + [1, 2, blocks]

    def crosses(t, way):
        if not ghosts:
            return True
        return jnp.logical_not(own_ghost & (way == across) & (t >= 2))

    low = jnp.full((tiles, LANES), low_ref[0], jnp.int32).astype(jnp.float32) / 4.0
    high = jnp.full((tiles, LANES), high_ref[0], jnp.int32).astype(jnp.float32) / 4.0
    centre = (high + low) / 2.0
    half = (high - low) / 2.0
    spread = centre / half
    ratio = 1.0 / spread
    coef[0, 0] = jnp.zeros((tiles, LANES), jnp.float32)
    coef[0, 1] = 1.0 / centre
    for t in range(1, STEPS):
        ahead = 1.0 / (2.0 * spread - ratio)
        coef[t, 0] = ahead * ratio
        coef[t, 1] = 2.0 * ahead / half
        ratio = ahead

    def index(cols, cols_flat, lane_of, tile_of, before, here, after):
        for c in range(tiles):
            cols_flat[pl.ds(c * 8, blocks), :] = cols[:, c * LANES:(c + 1) * LANES]
        for k in range(1, blocks):
            plane = {1: before, 2: after}.get(k, here)
            local = cols_flat[pl.ds(k, tiles, stride=8), :] - plane * rows
            lane_of[k] = local & (LANES - 1)
            tile_of[k] = local >> 7

    load_cols.wait()
    index(cols, cols_flat, lane_of, tile_of, previous, me, following)

    def taken(source, k, lane_of=lane_of, tile_of=tile_of):
        lanes, tile = lane_of[k], tile_of[k]
        out = [None] * comp
        for r in range(tiles):
            here = tile == r
            for j in range(comp):
                row = jnp.broadcast_to(source[pl.ds(r * comp + j, 1), :], (tiles, LANES))
                got = gather_lanes(row, lanes)
                out[j] = got if r == 0 else jnp.where(here, got, out[j])
        return out

    def combine(k, got, total, values=values):
        total = list(total)
        for i in range(comp):
            base = (k * comp + i) * comp * tiles
            for j in range(comp):
                total[i] = total[i] - values[pl.ds(base + j, tiles, stride=comp), :] * got[j]
        return total

    def own_part(t, residual):
        source = field.at[t]
        direct = [source[pl.ds(j, tiles, stride=comp), :] for j in range(comp)]
        residual = combine(0, direct, residual)
        for k in own[1:]:
            residual = combine(k, taken(source, k), residual)
        return direct, residual

    def far_part(t, residual):
        for way in (even, across):
            @pl.when(crosses(t, way))
            def _():
                send(t, field.at[t], way).wait_recv()
            residual = combine(1 + way, taken(beside.at[t, way], 1 + way), residual)
        return residual

    load_rhs.wait()
    for k in own + [1, 2]:
        load_values(k).wait()

    if ghosts:
        ghost_residual[...] = jnp.zeros(ghost_residual.shape, jnp.float32)

        for side, first in ((1, FIRST_EVEN), (0, FIRST_ODD)):
            @pl.when(own_ghost & (even == side))
            def _():
                for k in given[:first]:
                    give(k).start()

    def ghost_step(t):
        @pl.when(t == 1)
        def _():
            for k in given:
                give(k).wait_recv()
            here, past = outer, jnp.where(even == 1, ahead_of(me, devices - 2, devices), ahead_of(me, 2, devices))
            before = jnp.where(even == 1, past, me)
            after = jnp.where(even == 1, me, past)
            index(ghost_cols, ghost_flat, ghost_lane, ghost_tile, before, here, after)
            for j in range(comp):
                ghost_residual[j] = centre * beside[1, across, pl.ds(j, tiles, stride=comp), :]

        source = beside.at[t, across]
        direct = [source[pl.ds(j, tiles, stride=comp), :] for j in range(comp)]
        total = [ghost_residual[j] for j in range(comp)]
        total = combine(0, direct, total, ghost_values)
        for k in own[1:]:
            total = combine(k, taken(source, k, ghost_lane, ghost_tile), total, ghost_values)
        k = 2 - across
        total = combine(k, taken(field.at[t], k, ghost_lane, ghost_tile), total, ghost_values)
        feed(t).wait_recv()
        k = 1 + across
        total = combine(k, taken(beyond.at[t], k, ghost_lane, ghost_tile), total, ghost_values)
        for j in range(comp):
            ghost_residual[j] = total[j]
            beside[t + 1, across, pl.ds(j, tiles, stride=comp), :] = (
                coef[t, 0] * direct[j] + coef[t, 1] * total[j]
            )

    def step(t, carry):
        smoothed, residual = carry
        direct, residual = own_part(t, residual)
        smoothed = [s + d for s, d in zip(smoothed, direct)]
        residual = far_part(t, residual)
        for j in range(comp):
            field[t + 1, pl.ds(j, tiles, stride=comp), :] = (
                coef[t, 0] * direct[j] + coef[t, 1] * residual[j]
            )
        for way in range(2):
            @pl.when(crosses(t + 1, 1 - way))
            def _():
                send(t + 1, field.at[t + 1], way).start()
        if ghosts:
            for side, first in ((1, FIRST_EVEN), (0, FIRST_ODD)):
                if first <= blocks:
                    @pl.when(own_ghost & (even == side) & (t == 0))
                    def _():
                        for k in given[first:]:
                            give(k).start()

            @pl.when(feeds & (t + 1 < STEPS))
            def _():
                feed(t + 1).start()

            @pl.when(own_ghost & (t >= 1) & (t < STEPS))
            def _():
                ghost_step(t)
        return smoothed, residual

    smoothed = [jnp.zeros((tiles, LANES), jnp.float32) for j in range(comp)]
    residual = [rhs[pl.ds(j, tiles, stride=comp), :] for j in range(comp)]
    smoothed, residual = lax.fori_loop(0, STEPS, step, (smoothed, residual))

    direct, residual = own_part(STEPS, residual)
    for j in range(comp):
        smoothed_out[pl.ds(j, tiles, stride=comp), :] = smoothed[j] + direct[j]
    residual = far_part(STEPS, residual)

    squares = residual[0] * residual[0]
    for j in range(1, comp):
        squares = squares + residual[j] * residual[j]
    partial = jnp.sum(squares, axis=0, keepdims=True)

    def spread_sums(sums, slot, partner, sems):
        return pltpu.make_async_remote_copy(
            src_ref=sums.at[slot],
            dst_ref=sums.at[slot],
            send_sem=sems.at[0],
            recv_sem=sems.at[1],
            device_id=partner,
            device_id_type=MESH,
        )

    def wait_sends():
        for t in range(STEPS + 1):
            for way in range(2):
                @pl.when(crosses(t, 1 - way))
                def _():
                    send(t, field.at[t], way).wait_send()
        if ghosts:
            @pl.when(feeds)
            def _():
                for t in range(1, STEPS):
                    feed(t).wait_send()

            @pl.when(own_ghost)
            def _():
                for k in range(blocks + 1):
                    give(k).wait_send()

    near_sums[near_me] = partial
    for partner in near_partners:
        spread_sums(near_sums, near_me, partner, near_sems).start()
    for j in range(comp):
        residual_out[pl.ds(j, tiles, stride=comp), :] = residual[j]
    wait_sends()
    if near_partners:
        every = pl.ds(0, len(near_partners))
        spread_sums(near_sums, every, near_partners[0], near_sems).wait_send()
        spread_sums(near_sums, every, near_partners[0], near_sems).wait_recv()
    total = jnp.sum(near_sums[...], axis=0)
    if far_partners:
        far_sums[sub] = total
        for partner in far_partners:
            spread_sums(far_sums, sub, partner, far_sems).start()
        every = pl.ds(0, len(far_partners))
        spread_sums(far_sums, every, far_partners[0], far_sems).wait_send()
        spread_sums(far_sums, every, far_partners[0], far_sems).wait_recv()
        total = jnp.sum(far_sums[...], axis=0)
    count = float(comp * rows * devices)
    rms_ref[...] = jnp.broadcast_to(jnp.sqrt(jnp.sum(total, axis=1, keepdims=True) / count + 1e-06), rms_ref.shape)


def put_out(*refs):
    count = len(refs) // 2
    sems = refs[-1]
    copies = [
        pltpu.make_async_copy(refs[i] if i < 2 else refs[i].at[pl.ds(0, 1)], refs[count + i], sems.at[i]) for i in range(count)
    ]
    for copy in copies:
        copy.start()
    for copy in copies:
        copy.wait()


def flat(field, tiles):
    comp = field.shape[-2]
    lead = field.shape[:-2]
    cut = field.reshape(lead + (comp, tiles, LANES))
    return jnp.swapaxes(cut, -3, -2).reshape(-1, LANES)


def unflat(field, comp):
    tiles = field.shape[0] // comp
    return jnp.swapaxes(field.reshape(tiles, comp, LANES), 0, 1).reshape(comp, tiles * LANES)


def shards(subs, aggs, block_values, block_cols, coarse_rhs, guess, bound_low, bound_high):
    blocks, comp, _, rows = block_values.shape
    tiles = rows // LANES
    devices = subs * aggs
    near, far = (devices, 1) if devices <= ONE_ROUND else (aggs, subs)
    f32 = jnp.float32
    plane = (tiles * comp, LANES)
    anywhere = pl.BlockSpec(memory_space=pl.ANY)
    in_vmem = pl.BlockSpec(memory_space=pltpu.VMEM)
    in_hbm = pl.BlockSpec(memory_space=pltpu.HBM)
    dma = pltpu.SemaphoreType.DMA
    smoothed, residual, rms = pl.pallas_call(
        functools.partial(kernel, subs, aggs, (blocks, comp, tiles)),
        out_shape=(
            jax.ShapeDtypeStruct(plane, f32),
            jax.ShapeDtypeStruct(plane, f32),
            jax.ShapeDtypeStruct((8, LANES), f32),
        ),
        in_specs=[in_hbm] * 4 + [pl.BlockSpec(memory_space=pltpu.SMEM)] * 2,
        out_specs=(in_vmem,) * 3,
        scratch_shapes=[
            pltpu.VMEM((blocks * comp * comp * tiles, LANES), f32),
            pltpu.VMEM((blocks, rows), jnp.int32),
            pltpu.VMEM((8 * tiles, LANES), jnp.int32),
            pltpu.VMEM(plane, f32),
            pltpu.VMEM((STEPS + 1,) + plane, f32),
            pltpu.VMEM((STEPS + 1, 2) + plane, f32),
            pltpu.VMEM((blocks, tiles, LANES), jnp.int32),
            pltpu.VMEM((blocks, tiles, LANES), jnp.int32),
            pltpu.VMEM((STEPS, 2, tiles, LANES), f32),
            pltpu.VMEM((near, 1, LANES), f32),
            pltpu.VMEM((far, 1, LANES), f32),
            pltpu.VMEM((blocks * comp * comp * tiles, LANES), f32),
            pltpu.VMEM((blocks, rows), jnp.int32),
            pltpu.VMEM((8 * tiles, LANES), jnp.int32),
            pltpu.VMEM((blocks, tiles, LANES), jnp.int32),
            pltpu.VMEM((blocks, tiles, LANES), jnp.int32),
            pltpu.VMEM((comp, tiles, LANES), f32),
            pltpu.VMEM((STEPS + 1,) + plane, f32),
            dma((blocks,)),
            dma((5,)),
            dma((STEPS + 1, 2)),
            dma((STEPS + 1, 2)),
            dma((2,)),
            dma((2,)),
            dma((blocks + 1,)),
            dma((blocks + 1,)),
            dma((STEPS + 1,)),
            dma((STEPS + 1,)),
        ],
        compiler_params=pltpu.CompilerParams(collective_id=0, has_side_effects=True, vmem_limit_bytes=8 * 1024 * 1024),
    )(
        *[
            pltpu.with_memory_space_constraint(x, pltpu.HBM)
            for x in (
                flat(block_values, tiles), block_cols, flat(coarse_rhs, tiles), flat(guess, tiles),
            )
        ],
        bound_low, bound_high,
    )
    smoothed, residual, rms = pl.pallas_call(
        put_out,
        out_shape=(
            jax.ShapeDtypeStruct(plane, f32),
            jax.ShapeDtypeStruct(plane, f32),
            jax.ShapeDtypeStruct((1, LANES), f32),
        ),
        in_specs=[anywhere] * 3,
        out_specs=(anywhere,) * 3,
        scratch_shapes=[dma((3,))],
        compiler_params=pltpu.CompilerParams(vmem_limit_bytes=8 * 1024 * 1024),
    )(smoothed, residual, rms)
    return unflat(smoothed, comp), unflat(residual, comp), rms[0,:1]


def solution(mesh):
    split = ("sub", "agg")
    return jax.shard_map(
        functools.partial(shards, mesh.shape["sub"], mesh.shape["agg"]),
        mesh=mesh,
        in_specs=(
            P(None, None, None, split),
            P(None, split),
            P(None, split),
            P(None, split),
            P(),
            P(),
        ),
        out_specs=(P(None, split), P(None, split), P()),
        check_vma=False,
    )
```

```python
import functools

import jax
import jax.numpy as jnp
from jax import lax
from jax.experimental import pallas as pl
from jax.experimental.pallas import tpu as pltpu
from jax.sharding import PartitionSpec as P

STEPS = 4
ONE_ROUND = 32
LANES = 128
MESH = pl.DeviceIdType.MESH


def gather_lanes(rows, index):
    return jnp.take_along_axis(rows, index, axis=1, mode="promise_in_bounds")


def kernel(
    subs, aggs, shape,
    values_hbm, cols_hbm, rhs_hbm, guess_hbm, low_ref, high_ref,
    smoothed_out, residual_out, rms_ref,
    values, cols, cols_flat, rhs, field, beside, lane_of, tile_of, coef,
    near_sums, far_sums,
    ghost_values, ghost_lane, ghost_tile, part, ghost_part,
    values_sem, load_sem, send_sem, recv_sem,
    near_sems, far_sems,
    ghost_send, ghost_recv, part_send, part_recv,
):
    blocks, comp, tiles = shape
    devices = subs * aggs
    rows = tiles * LANES
    load_cols = pltpu.make_async_copy(cols_hbm, cols, load_sem.at[0])
    load_guess = pltpu.make_async_copy(guess_hbm, field.at[0], load_sem.at[1])
    load_rhs = pltpu.make_async_copy(rhs_hbm, rhs, load_sem.at[2])
    for load in (load_guess, load_cols):
        load.start()
    own = [0] + list(range(3, blocks))
    per_block = comp * comp * tiles

    def load_values(k):
        part = pl.ds(k * per_block, per_block)
        return pltpu.make_async_copy(values_hbm.at[part], values.at[part], values_sem.at[k])

    for k in own + [1, 2]:
        load_values(k).start()
    load_rhs.start()

    sub, agg = lax.axis_index("sub"), lax.axis_index("agg")
    me = sub * aggs + agg

    def ahead_of(place, by, size):
        to = place + by
        return jnp.where(to >= size, to - size, to)

    def beside_me(by_sub, by_agg):
        return (ahead_of(sub, by_sub, subs), ahead_of(agg, by_agg, aggs))

    def ring(way):
        turn = jnp.where(way == 0, agg == aggs - 1, agg == 0)
        to_sub = jnp.where(way == 0, ahead_of(sub, 1, subs), ahead_of(sub, subs - 1, subs))
        to_agg = jnp.where(way == 0, ahead_of(agg, 1, aggs), ahead_of(agg, aggs - 1, aggs))
        return (jnp.where(turn, to_sub, sub), to_agg)

    following = ahead_of(me, 1, devices)
    previous = ahead_of(me, devices - 1, devices)
    one_round = devices <= ONE_ROUND
    if one_round:
        near_steps = [(a, b) for a in range(subs) for b in range(aggs)][1:]
        near_steps.sort(key=lambda step: min(step[0], subs - step[0]))
        near, near_me = devices, me
        far_steps = []
    else:
        near_steps = [(0, b) for b in range(1, aggs)]
        near, near_me = aggs, agg
        far_steps = [(a, 0) for a in range(1, subs)]
    near_partners = [beside_me(a, b) for a, b in near_steps]
    far_partners = [beside_me(a, b) for a, b in far_steps]

    even = 1 - lax.rem(me, 2)
    across = 1 - even

    barrier = pltpu.get_barrier_semaphore()
    partners = far_partners + near_partners
    if not one_round:
        partners = [ring(0), ring(1)] + partners
    for partner in partners:
        pl.semaphore_signal(barrier, inc=1, device_id=partner, device_id_type=MESH)

    load_guess.wait()
    pl.semaphore_wait(barrier, len(partners))

    def send(step, source, way):
        return pltpu.make_async_remote_copy(
            src_ref=source,
            dst_ref=beside.at[step, way],
            send_sem=send_sem.at[step, way],
            recv_sem=recv_sem.at[step, way],
            device_id=ring(way),
            device_id_type=MESH,
        )

    for way in range(2):
        send(0, field.at[0], way).start()

    def give(i):
        source, target = (
            (values.at[pl.ds((1 + across) * per_block, per_block)], ghost_values),
            (lane_of.at[1 + across], ghost_lane),
            (tile_of.at[1 + across], ghost_tile),
        )[i]
        return pltpu.make_async_remote_copy(
            src_ref=source,
            dst_ref=target,
            send_sem=ghost_send.at[i],
            recv_sem=ghost_recv.at[i],
            device_id=ring(even),
            device_id_type=MESH,
        )

    def give_part(t):
        return pltpu.make_async_remote_copy(
            src_ref=part.at[t],
            dst_ref=ghost_part.at[t],
            send_sem=part_send.at[t],
            recv_sem=part_recv.at[t],
            device_id=ring(even),
            device_id_type=MESH,
        )

    low = jnp.full((tiles, LANES), low_ref[0], jnp.int32).astype(jnp.float32) / 4.0
    high = jnp.full((tiles, LANES), high_ref[0], jnp.int32).astype(jnp.float32) / 4.0
    centre = (high + low) / 2.0
    half = (high - low) / 2.0
    spread = centre / half
    ratio = 1.0 / spread
    coef[0, 0] = jnp.zeros((tiles, LANES), jnp.float32)
    coef[0, 1] = 1.0 / centre
    for t in range(1, STEPS):
        ahead = 1.0 / (2.0 * spread - ratio)
        coef[t, 0] = ahead * ratio
        coef[t, 1] = 2.0 * ahead / half
        ratio = ahead

    load_cols.wait()
    for c in range(tiles):
        cols_flat[pl.ds(c * 8, blocks), :] = cols[:, c * LANES:(c + 1) * LANES]
    for k in range(1, blocks):
        plane = {1: previous, 2: following}.get(k, me)
        local = cols_flat[pl.ds(k, tiles, stride=8), :] - plane * rows
        lane_of[k] = local & (LANES - 1)
        tile_of[k] = local >> 7

    def taken(source, lanes, tile):
        out = [None] * comp
        for r in range(tiles):
            here = tile == r
            for j in range(comp):
                row = jnp.broadcast_to(source[pl.ds(r * comp + j, 1), :], (tiles, LANES))
                got = gather_lanes(row, lanes)
                out[j] = got if r == 0 else jnp.where(here, got, out[j])
        return out

    def combine(k, got, total, values=values):
        total = list(total)
        for i in range(comp):
            base = (k * comp + i) * comp * tiles
            for j in range(comp):
                total[i] = total[i] - values[pl.ds(base + j, tiles, stride=comp), :] * got[j]
        return total

    def own_part(t, residual):
        source = field.at[t]
        direct = [source[pl.ds(j, tiles, stride=comp), :] for j in range(comp)]
        residual = combine(0, direct, residual)
        for k in own[1:]:
            residual = combine(k, taken(source, lane_of[k], tile_of[k]), residual)
        return direct, residual

    def far_part(t, way, residual):
        k = 1 + way
        return combine(k, taken(beside.at[t, way], lane_of[k], tile_of[k]), residual)

    def arrive(t, way):
        send(t, field.at[t], way).wait_recv()

    def advance(t, direct, residual):
        for j in range(comp):
            field[t + 1, pl.ds(j, tiles, stride=comp), :] = (
                coef[t, 0] * direct[j] + coef[t, 1] * residual[j]
            )

    load_rhs.wait()
    for k in own + [1, 2]:
        load_values(k).wait()
    for i in range(3):
        give(i).start()

    def two_steps(pair, carry):
        smoothed, residual = carry
        t = 2 * pair
        direct, residual = own_part(t, residual)
        smoothed = [s + d for s, d in zip(smoothed, direct)]
        arrive(t, even)
        residual = far_part(t, even, residual)
        for j in range(comp):
            part[pair, pl.ds(j, tiles, stride=comp), :] = residual[j]
        give_part(pair).start()
        arrive(t, across)
        residual = far_part(t, across, residual)
        advance(t, direct, residual)
        send(t + 1, field.at[t + 1], across).start()

        direct, residual = own_part(t + 1, residual)
        smoothed = [s + d for s, d in zip(smoothed, direct)]

        @pl.when(pair == 0)
        def _():
            for i in range(3):
                give(i).wait_recv()
        give_part(pair).wait_recv()
        other = [ghost_part[pair, pl.ds(j, tiles, stride=comp), :] for j in range(comp)]
        other = combine(0, taken(field.at[t], ghost_lane[...], ghost_tile[...]), other, ghost_values)
        for j in range(comp):
            beside[t + 1, across, pl.ds(j, tiles, stride=comp), :] = (
                coef[t, 0] * beside[t, across, pl.ds(j, tiles, stride=comp), :] + coef[t, 1] * other[j]
            )
        residual = far_part(t + 1, across, residual)
        arrive(t + 1, even)
        residual = far_part(t + 1, even, residual)
        advance(t + 1, direct, residual)
        for way in (even, across):
            send(t + 2, field.at[t + 2], way).start()
        return smoothed, residual

    smoothed = [jnp.zeros((tiles, LANES), jnp.float32) for j in range(comp)]
    residual = [rhs[pl.ds(j, tiles, stride=comp), :] for j in range(comp)]
    smoothed, residual = lax.fori_loop(0, STEPS // 2, two_steps, (smoothed, residual))

    direct, residual = own_part(STEPS, residual)
    for j in range(comp):
        smoothed_out[pl.ds(j, tiles, stride=comp), :] = smoothed[j] + direct[j]
    for way in (even, across):
        arrive(STEPS, way)
        residual = far_part(STEPS, way, residual)

    squares = residual[0] * residual[0]
    for j in range(1, comp):
        squares = squares + residual[j] * residual[j]
    partial = jnp.sum(squares, axis=0, keepdims=True)

    def spread_sums(sums, slot, partner, sems):
        return pltpu.make_async_remote_copy(
            src_ref=sums.at[slot],
            dst_ref=sums.at[slot],
            send_sem=sems.at[0],
            recv_sem=sems.at[1],
            device_id=partner,
            device_id_type=MESH,
        )

    def wait_sends():
        for t in range(STEPS + 1):
            send(t, field.at[t], across).wait_send()
            if t % 2 == 0:
                send(t, field.at[t], even).wait_send()
        for pair in range(STEPS // 2):
            give_part(pair).wait_send()
        for i in range(3):
            give(i).wait_send()

    near_sums[near_me] = partial
    for partner in near_partners:
        spread_sums(near_sums, near_me, partner, near_sems).start()
    for j in range(comp):
        residual_out[pl.ds(j, tiles, stride=comp), :] = residual[j]
    wait_sends()
    if near_partners:
        every = pl.ds(0, len(near_partners))
        spread_sums(near_sums, every, near_partners[0], near_sems).wait_send()
        spread_sums(near_sums, every, near_partners[0], near_sems).wait_recv()
    total = jnp.sum(near_sums[...], axis=0)
    if far_partners:
        far_sums[sub] = total
        for partner in far_partners:
            spread_sums(far_sums, sub, partner, far_sems).start()
        every = pl.ds(0, len(far_partners))
        spread_sums(far_sums, every, far_partners[0], far_sems).wait_send()
        spread_sums(far_sums, every, far_partners[0], far_sems).wait_recv()
        total = jnp.sum(far_sums[...], axis=0)
    count = float(comp * rows * devices)
    rms_ref[...] = jnp.broadcast_to(jnp.sqrt(jnp.sum(total, axis=1, keepdims=True) / count + 1e-06), rms_ref.shape)


def put_out(*refs):
    count = len(refs) // 2
    sems = refs[-1]
    copies = [
        pltpu.make_async_copy(refs[i] if i < 2 else refs[i].at[pl.ds(0, 1)], refs[count + i], sems.at[i]) for i in range(count)
    ]
    for copy in copies:
        copy.start()
    for copy in copies:
        copy.wait()


def flat(field, tiles):
    comp = field.shape[-2]
    lead = field.shape[:-2]
    cut = field.reshape(lead + (comp, tiles, LANES))
    return jnp.swapaxes(cut, -3, -2).reshape(-1, LANES)


def unflat(field, comp):
    tiles = field.shape[0] // comp
    return jnp.swapaxes(field.reshape(tiles, comp, LANES), 0, 1).reshape(comp, tiles * LANES)


def shards(subs, aggs, block_values, block_cols, coarse_rhs, guess, bound_low, bound_high):
    blocks, comp, _, rows = block_values.shape
    tiles = rows // LANES
    devices = subs * aggs
    near, far = (devices, 1) if devices <= ONE_ROUND else (aggs, subs)
    f32 = jnp.float32
    plane = (tiles * comp, LANES)
    anywhere = pl.BlockSpec(memory_space=pl.ANY)
    in_vmem = pl.BlockSpec(memory_space=pltpu.VMEM)
    in_hbm = pl.BlockSpec(memory_space=pltpu.HBM)
    dma = pltpu.SemaphoreType.DMA
    smoothed, residual, rms = pl.pallas_call(
        functools.partial(kernel, subs, aggs, (blocks, comp, tiles)),
        out_shape=(
            jax.ShapeDtypeStruct(plane, f32),
            jax.ShapeDtypeStruct(plane, f32),
            jax.ShapeDtypeStruct((8, LANES), f32),
        ),
        in_specs=[in_hbm] * 4 + [pl.BlockSpec(memory_space=pltpu.SMEM)] * 2,
        out_specs=(in_vmem,) * 3,
        scratch_shapes=[
            pltpu.VMEM((blocks * comp * comp * tiles, LANES), f32),
            pltpu.VMEM((blocks, rows), jnp.int32),
            pltpu.VMEM((8 * tiles, LANES), jnp.int32),
            pltpu.VMEM(plane, f32),
            pltpu.VMEM((STEPS + 1,) + plane, f32),
            pltpu.VMEM((STEPS + 1, 2) + plane, f32),
            pltpu.VMEM((blocks, tiles, LANES), jnp.int32),
            pltpu.VMEM((blocks, tiles, LANES), jnp.int32),
            pltpu.VMEM((STEPS, 2, tiles, LANES), f32),
            pltpu.VMEM((near, 1, LANES), f32),
            pltpu.VMEM((far, 1, LANES), f32),
            pltpu.VMEM((comp * comp * tiles, LANES), f32),
            pltpu.VMEM((tiles, LANES), jnp.int32),
            pltpu.VMEM((tiles, LANES), jnp.int32),
            pltpu.VMEM((STEPS // 2,) + plane, f32),
            pltpu.VMEM((STEPS // 2,) + plane, f32),
            dma((blocks,)),
            dma((5,)),
            dma((STEPS + 1, 2)),
            dma((STEPS + 1, 2)),
            dma((2,)),
            dma((2,)),
            dma((3,)),
            dma((3,)),
            dma((STEPS // 2,)),
            dma((STEPS // 2,)),
        ],
        compiler_params=pltpu.CompilerParams(collective_id=0, has_side_effects=True, vmem_limit_bytes=8 * 1024 * 1024),
    )(
        *[
            pltpu.with_memory_space_constraint(x, pltpu.HBM)
            for x in (
                flat(block_values, tiles), block_cols, flat(coarse_rhs, tiles), flat(guess, tiles),
            )
        ],
        bound_low, bound_high,
    )
    smoothed, residual, rms = pl.pallas_call(
        put_out,
        out_shape=(
            jax.ShapeDtypeStruct(plane, f32),
            jax.ShapeDtypeStruct(plane, f32),
            jax.ShapeDtypeStruct((1, LANES), f32),
        ),
        in_specs=[anywhere] * 3,
        out_specs=(anywhere,) * 3,
        scratch_shapes=[dma((3,))],
        compiler_params=pltpu.CompilerParams(vmem_limit_bytes=8 * 1024 * 1024),
    )(smoothed, residual, rms)
    return unflat(smoothed, comp), unflat(residual, comp), rms[0,:1]


def solution(mesh):
    split = ("sub", "agg")
    return jax.shard_map(
        functools.partial(shards, mesh.shape["sub"], mesh.shape["agg"]),
        mesh=mesh,
        in_specs=(
            P(None, None, None, split),
            P(None, split),
            P(None, split),
            P(None, split),
            P(),
            P(),
        ),
        out_specs=(P(None, split), P(None, split), P()),
        check_vma=False,
    )
```

```python
import functools

import jax
import jax.numpy as jnp
from jax import lax
from jax.experimental import pallas as pl
from jax.experimental.pallas import tpu as pltpu
from jax.sharding import PartitionSpec as P

STEPS = 4
ONE_ROUND = 32
LANES = 128
MESH = pl.DeviceIdType.MESH


def gather_lanes(rows, index):
    return jnp.take_along_axis(rows, index, axis=1, mode="promise_in_bounds")


def kernel(
    subs, aggs, shape,
    values_hbm, cols_hbm, rhs_hbm, guess_hbm, low_ref, high_ref,
    smoothed_out, residual_out, rms_ref,
    values, cols, cols_flat, rhs, field, beside, local_of, coef,
    near_sums, far_sums,
    ghost_values, ghost_local, ghost_residual, beyond, part, ghost_part,
    values_sem, load_sem, send_sem, recv_sem,
    near_sems, far_sems,
    ghost_send, ghost_recv, part_send, part_recv, beyond_send, beyond_recv,
):
    blocks, comp, tiles = shape
    devices = subs * aggs
    rows = tiles * LANES
    load_cols = pltpu.make_async_copy(cols_hbm, cols, load_sem.at[0])
    load_guess = pltpu.make_async_copy(guess_hbm, field.at[0], load_sem.at[1])
    load_rhs = pltpu.make_async_copy(rhs_hbm, rhs, load_sem.at[2])
    for load in (load_guess, load_cols):
        load.start()
    own = [0] + list(range(3, blocks))
    per_block = comp * comp * tiles

    def load_values(k):
        part = pl.ds(k * per_block, per_block)
        return pltpu.make_async_copy(values_hbm.at[part], values.at[part], values_sem.at[k])

    for k in own + [1, 2]:
        load_values(k).start()
    load_rhs.start()

    sub, agg = lax.axis_index("sub"), lax.axis_index("agg")
    me = sub * aggs + agg

    def ahead_of(place, by, size):
        to = place + by
        return jnp.where(to >= size, to - size, to)

    def beside_me(by_sub, by_agg):
        return (ahead_of(sub, by_sub, subs), ahead_of(agg, by_agg, aggs))

    def ring(way):
        turn = jnp.where(way == 0, agg == aggs - 1, agg == 0)
        to_sub = jnp.where(way == 0, ahead_of(sub, 1, subs), ahead_of(sub, subs - 1, subs))
        to_agg = jnp.where(way == 0, ahead_of(agg, 1, aggs), ahead_of(agg, aggs - 1, aggs))
        return (jnp.where(turn, to_sub, sub), to_agg)

    following = ahead_of(me, 1, devices)
    previous = ahead_of(me, devices - 1, devices)
    one_round = devices <= ONE_ROUND
    if one_round:
        near_steps = [(a, b) for a in range(subs) for b in range(aggs)][1:]
        near_steps.sort(key=lambda step: min(step[0], subs - step[0]))
        near, near_me = devices, me
        far_steps = []
    else:
        near_steps = [(0, b) for b in range(1, aggs)]
        near, near_me = aggs, agg
        far_steps = [(a, 0) for a in range(1, subs)]
    near_partners = [beside_me(a, b) for a, b in near_steps]
    far_partners = [beside_me(a, b) for a, b in far_steps]

    even = 1 - lax.rem(me, 2)
    across = 1 - even
    closing = one_round and devices >= 4
    first, last, feeds = me == 0, me == devices - 1, me == 1

    barrier = pltpu.get_barrier_semaphore()
    partners = far_partners + near_partners
    if not one_round:
        partners = [ring(0), ring(1)] + partners
    for partner in partners:
        pl.semaphore_signal(barrier, inc=1, device_id=partner, device_id_type=MESH)

    load_guess.wait()
    pl.semaphore_wait(barrier, len(partners))

    def send(step, source, way):
        return pltpu.make_async_remote_copy(
            src_ref=source,
            dst_ref=beside.at[step, way],
            send_sem=send_sem.at[step, way],
            recv_sem=recv_sem.at[step, way],
            device_id=ring(way),
            device_id_type=MESH,
        )

    for way in range(2):
        send(0, field.at[0], way).start()

    def over(source, target, i):
        return pltpu.make_async_remote_copy(
            src_ref=source,
            dst_ref=target,
            send_sem=ghost_send.at[i],
            recv_sem=ghost_recv.at[i],
            device_id=ring(even),
            device_id_type=MESH,
        )

    def give():
        k = 1 + across
        piece = pl.ds(k * per_block, per_block)
        return [
            over(values.at[piece], ghost_values.at[piece], 0),
            over(local_of.at[k], ghost_local.at[k], 1),
        ]

    def give_rest(i):
        k = 2 - across
        if i == 0:
            tail = pl.ds(3, blocks - 3)
            return [
                over(local_of.at[tail], ghost_local.at[tail], 2),
                over(local_of.at[k], ghost_local.at[k], 3),
            ]
        block = k if i == 2 else own[max(i - 2, 0)]
        piece = pl.ds(block * per_block, per_block)
        return [over(values.at[piece], ghost_values.at[piece], 3 + i)]

    pieces = blocks

    def give_more(*which):
        if closing and which:
            @pl.when(first & which[0])
            def _():
                for i in which[1:]:
                    for copy in give_rest(i):
                        copy.start()

    def feed(t):
        return pltpu.make_async_remote_copy(
            src_ref=field.at[t],
            dst_ref=beyond.at[t],
            send_sem=beyond_send.at[t],
            recv_sem=beyond_recv.at[t],
            device_id=((devices - 1) // aggs, (devices - 1) % aggs),
            device_id_type=MESH,
        )

    def give_part(t):
        return pltpu.make_async_remote_copy(
            src_ref=part.at[t],
            dst_ref=ghost_part.at[t],
            send_sem=part_send.at[t],
            recv_sem=part_recv.at[t],
            device_id=ring(even),
            device_id_type=MESH,
        )

    low = jnp.full((tiles, LANES), low_ref[0], jnp.int32).astype(jnp.float32) / 4.0
    high = jnp.full((tiles, LANES), high_ref[0], jnp.int32).astype(jnp.float32) / 4.0
    centre = (high + low) / 2.0
    half = (high - low) / 2.0
    spread = centre / half
    ratio = 1.0 / spread
    coef[0, 0] = jnp.zeros((tiles, LANES), jnp.float32)
    coef[0, 1] = 1.0 / centre
    for t in range(1, STEPS):
        ahead = 1.0 / (2.0 * spread - ratio)
        coef[t, 0] = ahead * ratio
        coef[t, 1] = 2.0 * ahead / half
        ratio = ahead

    load_cols.wait()
    for c in range(tiles):
        cols_flat[pl.ds(c * 8, blocks), :] = cols[:, c * LANES:(c + 1) * LANES]
    for k in range(1, blocks):
        plane = {1: previous, 2: following}.get(k, me)
        local_of[k] = cols_flat[pl.ds(k, tiles, stride=8), :] - plane * rows

    def taken(source, local):
        lanes, tile = local & (LANES - 1), local >> 7
        out = [None] * comp
        for r in range(tiles):
            here = tile == r
            for j in range(comp):
                row = jnp.broadcast_to(source[pl.ds(r * comp + j, 1), :], (tiles, LANES))
                got = gather_lanes(row, lanes)
                out[j] = got if r == 0 else jnp.where(here, got, out[j])
        return out

    def combine(k, got, total, values=values):
        total = list(total)
        for i in range(comp):
            base = (k * comp + i) * comp * tiles
            for j in range(comp):
                total[i] = total[i] - values[pl.ds(base + j, tiles, stride=comp), :] * got[j]
        return total

    def own_part(t, residual):
        source = field.at[t]
        direct = [source[pl.ds(j, tiles, stride=comp), :] for j in range(comp)]
        residual = combine(0, direct, residual)
        for k in own[1:]:
            residual = combine(k, taken(source, local_of[k]), residual)
        return direct, residual

    def far_part(t, way, residual):
        k = 1 + way
        return combine(k, taken(beside.at[t, way], local_of[k]), residual)

    def arrive(t, way):
        send(t, field.at[t], way).wait_recv()

    def advance(t, direct, residual):
        for j in range(comp):
            field[t + 1, pl.ds(j, tiles, stride=comp), :] = (
                coef[t, 0] * direct[j] + coef[t, 1] * residual[j]
            )

    load_rhs.wait()
    for k in own + [1, 2]:
        load_values(k).wait()
    for copy in give():
        copy.start()

    def foresee(t, total):
        source = beside.at[t, across]
        for j in range(comp):
            ghost_residual[pl.ds(j, tiles, stride=comp), :] = total[j]
            beside[t + 1, across, pl.ds(j, tiles, stride=comp), :] = (
                coef[t, 0] * source[pl.ds(j, tiles, stride=comp), :] + coef[t, 1] * total[j]
            )

    def foresee_alone(t):
        source = beside.at[t, across]
        total = [ghost_residual[pl.ds(j, tiles, stride=comp), :] for j in range(comp)]
        direct = [source[pl.ds(j, tiles, stride=comp), :] for j in range(comp)]
        total = combine(0, direct, total, ghost_values)
        for k in own[1:]:
            total = combine(k, taken(source, ghost_local[k]), total, ghost_values)
        k = 2 - across
        total = combine(k, taken(field.at[t], ghost_local[k]), total, ghost_values)
        feed(t).wait_recv()
        k = 1 + across
        total = combine(k, taken(beyond.at[t], ghost_local[k]), total, ghost_values)
        foresee(t, total)

    def two_steps(pair, carry):
        smoothed, residual = carry
        t = 2 * pair
        again = pair > 0
        direct, residual = own_part(t, residual)
        smoothed = [s + d for s, d in zip(smoothed, direct)]
        arrive(t, even)
        residual = far_part(t, even, residual)

        for j in range(comp):
            part[pair, pl.ds(j, tiles, stride=comp), :] = residual[j]
        give_part(pair).start()
        give_more(pair == 0, 0, 1)
        give_more(again, 6)
        arrive(t, across)
        residual = far_part(t, across, residual)
        advance(t, direct, residual)
        send(t + 1, field.at[t + 1], across).start()
        if closing:
            @pl.when(feeds & again)
            def _():
                feed(t + 1).start()
        give_more(pair == 0, 2)

        direct, residual = own_part(t + 1, residual)
        smoothed = [s + d for s, d in zip(smoothed, direct)]

        @pl.when(pair == 0)
        def _():
            for copy in give():
                copy.wait_recv()

        give_part(pair).wait_recv()
        other = [ghost_part[pair, pl.ds(j, tiles, stride=comp), :] for j in range(comp)]
        k = 2 - across
        foresee(t, combine(k, taken(field.at[t], ghost_local[k]), other, ghost_values))
        give_more(pair == 0, 3)
        residual = far_part(t + 1, across, residual)
        arrive(t + 1, even)
        residual = far_part(t + 1, even, residual)
        advance(t + 1, direct, residual)
        send(t + 2, field.at[t + 2], across).start()

        @pl.when(jnp.logical_not(first & again) if closing else True)
        def _():
            send(t + 2, field.at[t + 2], even).start()
        give_more(pair == 0, 4, 5)
        return smoothed, residual

    smoothed = [jnp.zeros((tiles, LANES), jnp.float32) for j in range(comp)]
    residual = [rhs[pl.ds(j, tiles, stride=comp), :] for j in range(comp)]
    smoothed, residual = lax.fori_loop(0, STEPS // 2, two_steps, (smoothed, residual))

    direct, residual = own_part(STEPS, residual)
    for j in range(comp):
        smoothed_out[pl.ds(j, tiles, stride=comp), :] = smoothed[j] + direct[j]
    arrive(STEPS, even)
    residual = far_part(STEPS, even, residual)

    @pl.when(jnp.logical_not(last) if closing else True)
    def _():
        arrive(STEPS, across)
    if closing:
        @pl.when(last)
        def _():
            for i in range(pieces):
                for copy in give_rest(i):
                    copy.wait_recv()
            foresee_alone(STEPS - 1)
    residual = far_part(STEPS, across, residual)

    squares = residual[0] * residual[0]
    for j in range(1, comp):
        squares = squares + residual[j] * residual[j]
    partial = jnp.sum(squares, axis=0, keepdims=True)

    def spread_sums(sums, slot, partner, sems):
        return pltpu.make_async_remote_copy(
            src_ref=sums.at[slot],
            dst_ref=sums.at[slot],
            send_sem=sems.at[0],
            recv_sem=sems.at[1],
            device_id=partner,
            device_id_type=MESH,
        )

    def wait_sends():
        for t in range(STEPS + 1):
            send(t, field.at[t], across).wait_send()
            if t % 2 == 0:
                @pl.when(jnp.logical_not(first) if closing and t == STEPS else True)
                def _():
                    send(t, field.at[t], even).wait_send()
        for pair in range(STEPS // 2):
            give_part(pair).wait_send()
        for copy in give():
            copy.wait_send()
        if closing:
            @pl.when(first)
            def _():
                for i in range(pieces):
                    for copy in give_rest(i):
                        copy.wait_send()

            @pl.when(feeds)
            def _():
                feed(STEPS - 1).wait_send()

    near_sums[near_me] = partial
    for partner in near_partners:
        spread_sums(near_sums, near_me, partner, near_sems).start()
    for j in range(comp):
        residual_out[pl.ds(j, tiles, stride=comp), :] = residual[j]
    wait_sends()
    if near_partners:
        every = pl.ds(0, len(near_partners))
        spread_sums(near_sums, every, near_partners[0], near_sems).wait_send()
        spread_sums(near_sums, every, near_partners[0], near_sems).wait_recv()
    total = jnp.sum(near_sums[...], axis=0)
    if far_partners:
        far_sums[sub] = total
        for partner in far_partners:
            spread_sums(far_sums, sub, partner, far_sems).start()
        every = pl.ds(0, len(far_partners))
        spread_sums(far_sums, every, far_partners[0], far_sems).wait_send()
        spread_sums(far_sums, every, far_partners[0], far_sems).wait_recv()
        total = jnp.sum(far_sums[...], axis=0)
    count = float(comp * rows * devices)
    rms_ref[...] = jnp.broadcast_to(jnp.sqrt(jnp.sum(total, axis=1, keepdims=True) / count + 1e-06), rms_ref.shape)


def put_out(*refs):
    count = len(refs) // 2
    sems = refs[-1]
    copies = [
        pltpu.make_async_copy(refs[i] if i < 2 else refs[i].at[pl.ds(0, 1)], refs[count + i], sems.at[i]) for i in range(count)
    ]
    for copy in copies:
        copy.start()
    for copy in copies:
        copy.wait()


def flat(field, tiles):
    comp = field.shape[-2]
    lead = field.shape[:-2]
    cut = field.reshape(lead + (comp, tiles, LANES))
    return jnp.swapaxes(cut, -3, -2).reshape(-1, LANES)


def unflat(field, comp):
    tiles = field.shape[0] // comp
    return jnp.swapaxes(field.reshape(tiles, comp, LANES), 0, 1).reshape(comp, tiles * LANES)


def shards(subs, aggs, block_values, block_cols, coarse_rhs, guess, bound_low, bound_high):
    blocks, comp, _, rows = block_values.shape
    tiles = rows // LANES
    devices = subs * aggs
    near, far = (devices, 1) if devices <= ONE_ROUND else (aggs, subs)
    f32 = jnp.float32
    plane = (tiles * comp, LANES)
    anywhere = pl.BlockSpec(memory_space=pl.ANY)
    in_vmem = pl.BlockSpec(memory_space=pltpu.VMEM)
    in_hbm = pl.BlockSpec(memory_space=pltpu.HBM)
    dma = pltpu.SemaphoreType.DMA
    smoothed, residual, rms = pl.pallas_call(
        functools.partial(kernel, subs, aggs, (blocks, comp, tiles)),
        out_shape=(
            jax.ShapeDtypeStruct(plane, f32),
            jax.ShapeDtypeStruct(plane, f32),
            jax.ShapeDtypeStruct((8, LANES), f32),
        ),
        in_specs=[in_hbm] * 4 + [pl.BlockSpec(memory_space=pltpu.SMEM)] * 2,
        out_specs=(in_vmem,) * 3,
        scratch_shapes=[
            pltpu.VMEM((blocks * comp * comp * tiles, LANES), f32),
            pltpu.VMEM((blocks, rows), jnp.int32),
            pltpu.VMEM((8 * tiles, LANES), jnp.int32),
            pltpu.VMEM(plane, f32),
            pltpu.VMEM((STEPS + 1,) + plane, f32),
            pltpu.VMEM((STEPS + 1, 2) + plane, f32),
            pltpu.VMEM((blocks, tiles, LANES), jnp.int32),
            pltpu.VMEM((STEPS, 2, tiles, LANES), f32),
            pltpu.VMEM((near, 1, LANES), f32),
            pltpu.VMEM((far, 1, LANES), f32),
            pltpu.VMEM((blocks * comp * comp * tiles, LANES), f32),
            pltpu.VMEM((blocks, tiles, LANES), jnp.int32),
            pltpu.VMEM(plane, f32),
            pltpu.VMEM((STEPS + 1,) + plane, f32),
            pltpu.VMEM((STEPS // 2,) + plane, f32),
            pltpu.VMEM((STEPS // 2,) + plane, f32),
            dma((blocks,)),
            dma((5,)),
            dma((STEPS + 1, 2)),
            dma((STEPS + 1, 2)),
            dma((2,)),
            dma((2,)),
            dma((blocks + 3,)),
            dma((blocks + 3,)),
            dma((STEPS // 2,)),
            dma((STEPS // 2,)),
            dma((STEPS + 1,)),
            dma((STEPS + 1,)),
        ],
        compiler_params=pltpu.CompilerParams(collective_id=0, has_side_effects=True, vmem_limit_bytes=8 * 1024 * 1024),
    )(
        *[
            pltpu.with_memory_space_constraint(x, pltpu.HBM)
            for x in (
                flat(block_values, tiles), block_cols, flat(coarse_rhs, tiles), flat(guess, tiles),
            )
        ],
        bound_low, bound_high,
    )
    smoothed, residual, rms = pl.pallas_call(
        put_out,
        out_shape=(
            jax.ShapeDtypeStruct(plane, f32),
            jax.ShapeDtypeStruct(plane, f32),
            jax.ShapeDtypeStruct((1, LANES), f32),
        ),
        in_specs=[anywhere] * 3,
        out_specs=(anywhere,) * 3,
        scratch_shapes=[dma((3,))],
        compiler_params=pltpu.CompilerParams(vmem_limit_bytes=8 * 1024 * 1024),
    )(smoothed, residual, rms)
    return unflat(smoothed, comp), unflat(residual, comp), rms[0,:1]


def solution(mesh):
    split = ("sub", "agg")
    return jax.shard_map(
        functools.partial(shards, mesh.shape["sub"], mesh.shape["agg"]),
        mesh=mesh,
        in_specs=(
            P(None, None, None, split),
            P(None, split),
            P(None, split),
            P(None, split),
            P(),
            P(),
        ),
        out_specs=(P(None, split), P(None, split), P()),
        check_vma=False,
    )
```

```python
import functools

import jax
import jax.numpy as jnp
from jax import lax
from jax.experimental import pallas as pl
from jax.experimental.pallas import tpu as pltpu
from jax.sharding import PartitionSpec as P

STEPS = 4
ONE_ROUND = 32
LANES = 128
MESH = pl.DeviceIdType.MESH


def gather_lanes(rows, index):
    return jnp.take_along_axis(rows, index, axis=1, mode="promise_in_bounds")


def kernel(
    subs, aggs, shape,
    values_hbm, cols_hbm, rhs_hbm, guess_hbm, low_ref, high_ref,
    smoothed_out, residual_out, rms_ref,
    values, cols, cols_flat, rhs, field, beside, local_of, coef,
    near_sums, far_sums,
    ghost_values, ghost_local, ghost_residual, beyond, part, ghost_part,
    load_sem, chip_sem, cross_sem, ghost_sem, sum_sem,
):
    blocks, comp, tiles = shape
    devices = subs * aggs
    rows = tiles * LANES
    load_cols = pltpu.make_async_copy(cols_hbm, cols, load_sem.at[0])
    load_guess = pltpu.make_async_copy(guess_hbm, field.at[0], load_sem.at[1])
    load_rhs = pltpu.make_async_copy(rhs_hbm, rhs, load_sem.at[3])
    load_values = pltpu.make_async_copy(values_hbm, values, load_sem.at[2])
    own = [0] + list(range(3, blocks))
    per_block = comp * comp * tiles


    sub, agg = lax.axis_index("sub"), lax.axis_index("agg")
    me = sub * aggs + agg

    def ahead_of(place, by, size):
        to = place + by
        return jnp.where(to >= size, to - size, to)

    def beside_me(by_sub, by_agg):
        return (ahead_of(sub, by_sub, subs), ahead_of(agg, by_agg, aggs))

    def ring(way):
        turn = jnp.where(way == 0, agg == aggs - 1, agg == 0)
        to_sub = jnp.where(way == 0, ahead_of(sub, 1, subs), ahead_of(sub, subs - 1, subs))
        to_agg = jnp.where(way == 0, ahead_of(agg, 1, aggs), ahead_of(agg, aggs - 1, aggs))
        return (jnp.where(turn, to_sub, sub), to_agg)

    following = ahead_of(me, 1, devices)
    previous = ahead_of(me, devices - 1, devices)
    one_round = devices <= ONE_ROUND
    if one_round:
        low = sub < subs // 2
        near_steps = [
            (jnp.where(low, subs - a, a), b) for a in range(1, subs) for b in range(aggs)
        ] + [(0, b) for b in range(1, aggs)]
        near, near_me = devices, me
        far_steps = []
    else:
        near_steps = [(0, b) for b in range(1, aggs)]
        near, near_me = aggs, agg
        far_steps = [(a, 0) for a in range(1, subs)]
    near_partners = [beside_me(a, b) for a, b in near_steps]
    far_partners = [beside_me(a, b) for a, b in far_steps]

    even = 1 - lax.rem(me, 2)
    across = 1 - even
    closing = one_round and devices >= 4
    first, last = me == 0, me == devices - 1
    gives = takes = first | last
    feeds = (me == 1) | (me == devices - 2)

    barrier = pltpu.get_barrier_semaphore()
    partners = far_partners + near_partners
    if not one_round:
        partners = [ring(0), ring(1)] + partners
    for partner in partners:
        pl.semaphore_signal(barrier, inc=1, device_id=partner, device_id_type=MESH)
    for load in (load_guess, load_cols, load_values, load_rhs):
        load.start()

    load_guess.wait()
    pl.semaphore_wait(barrier, len(partners))

    def send(step, source, way):
        return pltpu.make_async_remote_copy(
            src_ref=source,
            dst_ref=beside.at[step, way],
            send_sem=cross_sem.at[0] if way is even else chip_sem.at[0],
            recv_sem=(
                cross_sem.at[1 + lax.div(step, 2)] if way is even else chip_sem.at[1 + lax.rem(step, 2)]
            ),
            device_id=ring(way),
            device_id_type=MESH,
        )

    for way in (even, across):
        send(0, field.at[0], way).start()

    def over(source, target, i):
        return pltpu.make_async_remote_copy(
            src_ref=source,
            dst_ref=target,
            send_sem=ghost_sem.at[2 * i],
            recv_sem=ghost_sem.at[2 * i + 1],
            device_id=ring(even),
            device_id_type=MESH,
        )

    def give():
        k = 1 + across
        piece = pl.ds(k * per_block, per_block)
        return [
            over(values.at[piece], ghost_values.at[piece], 0),
            over(local_of.at[k], ghost_local.at[k], 0),
        ]

    def give_rest(i):
        k = 2 - across
        if i == 0:
            tail = pl.ds(3, blocks - 3)
            return [
                over(local_of.at[tail], ghost_local.at[tail], 1),
                over(local_of.at[k], ghost_local.at[k], 1),
            ]
        block = k if i == 2 else own[max(i - 2, 0)]
        piece = pl.ds(block * per_block, per_block)
        return [over(values.at[piece], ghost_values.at[piece], 1)]

    def given(count, i):
        some = pl.ds(0, count)
        return over(values.at[some], ghost_values.at[some], i)

    block_given = given(per_block + tiles, 0)
    rest_given = given((blocks - 1) * per_block + (blocks - 2) * tiles, 1)

    def give_more(*which):
        if closing and which:
            for giver, some in ((first, which[1]), (last, which[2])):
                if some:
                    @pl.when(giver & which[0])
                    def _():
                        for i in some:
                            for copy in give_rest(i):
                                copy.start()

    def feed(t):
        to = jnp.where(me == 1, devices - 1, 0)
        return pltpu.make_async_remote_copy(
            src_ref=field.at[t],
            dst_ref=beyond.at[t],
            send_sem=ghost_sem.at[4],
            recv_sem=ghost_sem.at[5],
            device_id=(to // aggs, lax.rem(to, aggs)),
            device_id_type=MESH,
        )

    def give_part(t):
        return pltpu.make_async_remote_copy(
            src_ref=part.at[t],
            dst_ref=ghost_part.at[t],
            send_sem=cross_sem.at[0],
            recv_sem=cross_sem.at[2 + STEPS // 2 + t],
            device_id=ring(even),
            device_id_type=MESH,
        )

    low = jnp.full((tiles, LANES), low_ref[0], jnp.int32).astype(jnp.float32) / 4.0
    high = jnp.full((tiles, LANES), high_ref[0], jnp.int32).astype(jnp.float32) / 4.0
    centre = (high + low) / 2.0
    half = (high - low) / 2.0
    spread = centre / half
    ratio = 1.0 / spread
    coef[0, 0] = jnp.zeros((tiles, LANES), jnp.float32)
    coef[0, 1] = 1.0 / centre
    for t in range(1, STEPS):
        ahead = 1.0 / (2.0 * spread - ratio)
        coef[t, 0] = ahead * ratio
        coef[t, 1] = 2.0 * ahead / half
        ratio = ahead

    load_cols.wait()
    for c in range(tiles):
        cols_flat[pl.ds(c * 8, blocks), :] = cols[:, c * LANES:(c + 1) * LANES]
    for k in range(1, blocks):
        plane = {1: previous, 2: following}.get(k, me)
        local_of[k] = cols_flat[pl.ds(k, tiles, stride=8), :] - plane * rows

    def taken(source, local):
        lanes, tile = local & (LANES - 1), local >> 7
        out = [None] * comp
        for r in range(tiles):
            here = tile == r
            for j in range(comp):
                row = jnp.broadcast_to(source[pl.ds(r * comp + j, 1), :], (tiles, LANES))
                got = gather_lanes(row, lanes)
                out[j] = got if r == 0 else jnp.where(here, got, out[j])
        return out

    def combine(k, got, total, values=values):
        total = list(total)
        for i in range(comp):
            base = (k * comp + i) * comp * tiles
            for j in range(comp):
                total[i] = total[i] - values[pl.ds(base + j, tiles, stride=comp), :] * got[j]
        return total

    def own_part(t, residual):
        source = field.at[t]
        direct = [source[pl.ds(j, tiles, stride=comp), :] for j in range(comp)]
        residual = combine(0, direct, residual)
        for k in own[1:]:
            residual = combine(k, taken(source, local_of[k]), residual)
        return direct, residual

    def far_part(t, way, residual):
        k = 1 + way
        return combine(k, taken(beside.at[t, way], local_of[k]), residual)

    def arrive(t, way):
        send(t, field.at[t], across if way is even else even).wait_recv()

    def advance(t, direct, residual):
        for j in range(comp):
            field[t + 1, pl.ds(j, tiles, stride=comp), :] = (
                coef[t, 0] * direct[j] + coef[t, 1] * residual[j]
            )

    load_rhs.wait()
    load_values.wait()
    for copy in give():
        copy.start()

    def foresee(t, total):
        source = beside.at[t, across]
        for j in range(comp):
            ghost_residual[pl.ds(j, tiles, stride=comp), :] = total[j]
            beside[t + 1, across, pl.ds(j, tiles, stride=comp), :] = (
                coef[t, 0] * source[pl.ds(j, tiles, stride=comp), :] + coef[t, 1] * total[j]
            )

    def foresee_alone(t):
        source = beside.at[t, across]
        total = [ghost_residual[pl.ds(j, tiles, stride=comp), :] for j in range(comp)]
        direct = [source[pl.ds(j, tiles, stride=comp), :] for j in range(comp)]
        total = combine(0, direct, total, ghost_values)
        for k in own[1:]:
            total = combine(k, taken(source, ghost_local[k]), total, ghost_values)
        k = 2 - across
        total = combine(k, taken(field.at[t], ghost_local[k]), total, ghost_values)
        feed(t).wait_recv()
        k = 1 + across
        total = combine(k, taken(beyond.at[t], ghost_local[k]), total, ghost_values)
        foresee(t, total)

    def two_steps(pair, carry):
        smoothed, residual = carry
        t = 2 * pair
        again = pair > 0
        direct, residual = own_part(t, residual)
        smoothed = [s + d for s, d in zip(smoothed, direct)]
        arrive(t, even)
        residual = far_part(t, even, residual)

        for j in range(comp):
            part[pair, pl.ds(j, tiles, stride=comp), :] = residual[j]
        give_part(pair).start()
        give_more(pair == 0, (0, 1), (0, 1))
        give_more(again, (5, 6), (5, 6))
        arrive(t, across)
        residual = far_part(t, across, residual)
        advance(t, direct, residual)
        send(t + 1, field.at[t + 1], across).start()
        if closing:
            @pl.when(feeds & again)
            def _():
                feed(t + 1).start()
        give_more(pair == 0, (2,), (2,))

        direct, residual = own_part(t + 1, residual)
        smoothed = [s + d for s, d in zip(smoothed, direct)]

        @pl.when(pair == 0)
        def _():
            block_given.wait_recv()

        give_part(pair).wait_recv()
        other = [ghost_part[pair, pl.ds(j, tiles, stride=comp), :] for j in range(comp)]
        k = 2 - across
        foresee(t, combine(k, taken(field.at[t], ghost_local[k]), other, ghost_values))
        give_more(pair == 0, (), ())
        residual = far_part(t + 1, across, residual)
        arrive(t + 1, even)
        residual = far_part(t + 1, even, residual)
        advance(t + 1, direct, residual)
        send(t + 2, field.at[t + 2], across).start()

        @pl.when(jnp.logical_not(gives & again) if closing else True)
        def _():
            send(t + 2, field.at[t + 2], even).start()
        give_more(pair == 0, (3, 4), (3, 4))
        return smoothed, residual

    smoothed = [jnp.zeros((tiles, LANES), jnp.float32) for j in range(comp)]
    residual = [rhs[pl.ds(j, tiles, stride=comp), :] for j in range(comp)]
    smoothed, residual = lax.fori_loop(0, STEPS // 2, two_steps, (smoothed, residual))

    direct, residual = own_part(STEPS, residual)
    for j in range(comp):
        smoothed_out[pl.ds(j, tiles, stride=comp), :] = smoothed[j] + direct[j]
    arrive(STEPS, even)
    residual = far_part(STEPS, even, residual)

    @pl.when(jnp.logical_not(takes) if closing else True)
    def _():
        arrive(STEPS, across)
    if closing:
        @pl.when(takes)
        def _():
            rest_given.wait_recv()
            foresee_alone(STEPS - 1)
    residual = far_part(STEPS, across, residual)

    squares = residual[0] * residual[0]
    for j in range(1, comp):
        squares = squares + residual[j] * residual[j]
    partial = jnp.sum(squares, axis=0, keepdims=True)

    def spread_sums(sums, slot, partner, sems):
        return pltpu.make_async_remote_copy(
            src_ref=sums.at[slot],
            dst_ref=sums.at[slot],
            send_sem=sems.at[0],
            recv_sem=sems.at[1],
            device_id=partner,
            device_id_type=MESH,
        )

    def sent(count, way):
        planes = pl.ds(0, count)
        return pltpu.make_async_remote_copy(
            src_ref=field.at[planes],
            dst_ref=beyond.at[planes],
            send_sem=cross_sem.at[0] if way is even else chip_sem.at[0],
            recv_sem=ghost_sem.at[5],
            device_id=ring(way),
            device_id_type=MESH,
        )

    def wait_sends():
        sent(STEPS + 1, across).wait_send()
        block_given.wait_send()

        @pl.when(jnp.logical_not(gives) if closing else True)
        def _():
            sent(STEPS + 1, even).wait_send()
        if closing:
            @pl.when(gives)
            def _():
                sent(STEPS, even).wait_send()
                rest_given.wait_send()

            @pl.when(feeds)
            def _():
                feed(STEPS - 1).wait_send()

    near_sums[near_me] = partial
    for partner in near_partners:
        spread_sums(near_sums, near_me, partner, sum_sem.at[pl.ds(0, 2)]).start()
    for j in range(comp):
        residual_out[pl.ds(j, tiles, stride=comp), :] = residual[j]
    wait_sends()
    if near_partners:
        every_near = pl.ds(0, len(near_partners))
        spread_sums(near_sums, every_near, near_partners[0], sum_sem.at[pl.ds(0, 2)]).wait_recv()
    total = jnp.sum(near_sums[...], axis=0)
    if far_partners:
        far_sums[sub] = total
        for partner in far_partners:
            spread_sums(far_sums, sub, partner, sum_sem.at[pl.ds(2, 2)]).start()
        every = pl.ds(0, len(far_partners))
        spread_sums(far_sums, every, far_partners[0], sum_sem.at[pl.ds(2, 2)]).wait_send()
        spread_sums(far_sums, every, far_partners[0], sum_sem.at[pl.ds(2, 2)]).wait_recv()
        total = jnp.sum(far_sums[...], axis=0)
    count = float(comp * rows * devices)
    rms_ref[...] = jnp.broadcast_to(jnp.sqrt(jnp.sum(total, axis=1, keepdims=True) / count + 1e-06), rms_ref.shape)
    if near_partners:
        spread_sums(near_sums, every_near, near_partners[0], sum_sem.at[pl.ds(0, 2)]).wait_send()


def put_out(*refs):
    count = len(refs) // 2
    sems = refs[-1]
    copies = [
        pltpu.make_async_copy(refs[i] if i < 2 else refs[i].at[pl.ds(0, 1)], refs[count + i], sems.at[i]) for i in range(count)
    ]
    for copy in copies:
        copy.start()
    for copy in copies:
        copy.wait()


def flat(field, tiles):
    comp = field.shape[-2]
    lead = field.shape[:-2]
    cut = field.reshape(lead + (comp, tiles, LANES))
    return jnp.swapaxes(cut, -3, -2).reshape(-1, LANES)


def unflat(field, comp):
    tiles = field.shape[0] // comp
    return jnp.swapaxes(field.reshape(tiles, comp, LANES), 0, 1).reshape(comp, tiles * LANES)


def shards(subs, aggs, block_values, block_cols, coarse_rhs, guess, bound_low, bound_high):
    blocks, comp, _, rows = block_values.shape
    tiles = rows // LANES
    devices = subs * aggs
    near, far = (devices, 1) if devices <= ONE_ROUND else (aggs, subs)
    f32 = jnp.float32
    plane = (tiles * comp, LANES)
    anywhere = pl.BlockSpec(memory_space=pl.ANY)
    in_vmem = pl.BlockSpec(memory_space=pltpu.VMEM)
    in_hbm = pl.BlockSpec(memory_space=pltpu.HBM)
    dma = pltpu.SemaphoreType.DMA
    smoothed, residual, rms = pl.pallas_call(
        functools.partial(kernel, subs, aggs, (blocks, comp, tiles)),
        out_shape=(
            jax.ShapeDtypeStruct(plane, f32),
            jax.ShapeDtypeStruct(plane, f32),
            jax.ShapeDtypeStruct((8, LANES), f32),
        ),
        in_specs=[in_hbm] * 4 + [pl.BlockSpec(memory_space=pltpu.SMEM)] * 2,
        out_specs=(in_vmem,) * 3,
        scratch_shapes=[
            pltpu.VMEM((blocks * comp * comp * tiles, LANES), f32),
            pltpu.VMEM((blocks, rows), jnp.int32),
            pltpu.VMEM((8 * tiles, LANES), jnp.int32),
            pltpu.VMEM(plane, f32),
            pltpu.VMEM((STEPS + 1,) + plane, f32),
            pltpu.VMEM((STEPS + 1, 2) + plane, f32),
            pltpu.VMEM((blocks, tiles, LANES), jnp.int32),
            pltpu.VMEM((STEPS, 2, tiles, LANES), f32),
            pltpu.VMEM((near, 1, LANES), f32),
            pltpu.VMEM((far, 1, LANES), f32),
            pltpu.VMEM((blocks * comp * comp * tiles, LANES), f32),
            pltpu.VMEM((blocks, tiles, LANES), jnp.int32),
            pltpu.VMEM(plane, f32),
            pltpu.VMEM((STEPS + 1,) + plane, f32),
            pltpu.VMEM((STEPS // 2,) + plane, f32),
            pltpu.VMEM((STEPS // 2,) + plane, f32),
            dma((4,)),
            dma((3,)),
            dma((2 + STEPS,)),
            dma((6,)),
            dma((2 if far == 1 else 4,)),
        ],
        compiler_params=pltpu.CompilerParams(collective_id=0, has_side_effects=True, vmem_limit_bytes=8 * 1024 * 1024),
    )(
        *[
            pltpu.with_memory_space_constraint(x, pltpu.HBM)
            for x in (
                flat(block_values, tiles), block_cols, flat(coarse_rhs, tiles), flat(guess, tiles),
            )
        ],
        bound_low, bound_high,
    )
    smoothed, residual, rms = pl.pallas_call(
        put_out,
        out_shape=(
            jax.ShapeDtypeStruct(plane, f32),
            jax.ShapeDtypeStruct(plane, f32),
            jax.ShapeDtypeStruct((1, LANES), f32),
        ),
        in_specs=[anywhere] * 3,
        out_specs=(anywhere,) * 3,
        scratch_shapes=[dma((3,))],
        compiler_params=pltpu.CompilerParams(vmem_limit_bytes=8 * 1024 * 1024),
    )(smoothed, residual, rms)
    return unflat(smoothed, comp), unflat(residual, comp), rms[0,:1]


def solution(mesh):
    split = ("sub", "agg")
    return jax.shard_map(
        functools.partial(shards, mesh.shape["sub"], mesh.shape["agg"]),
        mesh=mesh,
        in_specs=(
            P(None, None, None, split),
            P(None, split),
            P(None, split),
            P(None, split),
            P(),
            P(),
        ),
        out_specs=(P(None, split), P(None, split), P()),
        check_vma=False,
    )
```

```python
import functools

import jax
import jax.numpy as jnp
from jax import lax
from jax.experimental import pallas as pl
from jax.experimental.pallas import tpu as pltpu
from jax.sharding import PartitionSpec as P

STEPS = 4
ONE_ROUND = 32
LANES = 128
MESH = pl.DeviceIdType.MESH


def gather_lanes(rows, index):
    return jnp.take_along_axis(rows, index, axis=1, mode="promise_in_bounds")


def kernel(
    subs, aggs, shape,
    values_hbm, cols_hbm, rhs_hbm, guess_hbm, low_ref, high_ref,
    smoothed_out, residual_out, rms_ref,
    values, cols, cols_flat, rhs, field, beside, local_of, coef,
    near_sums, far_sums,
    ghost_values, ghost_local, ghost_residual, beyond, part, ghost_part,
    load_sem, chip_sem, cross_sem, ghost_sem, sum_sem,
):
    blocks, comp, tiles = shape
    devices = subs * aggs
    rows = tiles * LANES
    load_cols = pltpu.make_async_copy(cols_hbm, cols, load_sem.at[0])
    load_guess = pltpu.make_async_copy(guess_hbm, field.at[0], load_sem.at[1])
    load_rhs = pltpu.make_async_copy(rhs_hbm, rhs, load_sem.at[3])
    load_values = pltpu.make_async_copy(values_hbm, values, load_sem.at[2])
    own = [0] + list(range(3, blocks))
    per_block = comp * comp * tiles


    sub, agg = lax.axis_index("sub"), lax.axis_index("agg")
    me = sub * aggs + agg

    def ahead_of(place, by, size):
        to = place + by
        return jnp.where(to >= size, to - size, to)

    def beside_me(by_sub, by_agg):
        return (ahead_of(sub, by_sub, subs), ahead_of(agg, by_agg, aggs))

    def ring(way):
        turn = jnp.where(way == 0, agg == aggs - 1, agg == 0)
        to_sub = jnp.where(way == 0, ahead_of(sub, 1, subs), ahead_of(sub, subs - 1, subs))
        to_agg = jnp.where(way == 0, ahead_of(agg, 1, aggs), ahead_of(agg, aggs - 1, aggs))
        return (jnp.where(turn, to_sub, sub), to_agg)

    following = ahead_of(me, 1, devices)
    previous = ahead_of(me, devices - 1, devices)
    one_round = devices <= ONE_ROUND
    if one_round:
        low = sub < subs // 2
        near_steps = [
            (jnp.where(low, subs - a, a), b) for a in range(1, subs) for b in range(aggs)
        ] + [(0, b) for b in range(1, aggs)]
        near, near_me = devices, me
        far_steps = []
    else:
        near_steps = [(0, b) for b in range(1, aggs)]
        near, near_me = aggs, agg
        far_steps = [(a, 0) for a in range(1, subs)]
    near_partners = [beside_me(a, b) for a, b in near_steps]
    far_partners = [beside_me(a, b) for a, b in far_steps]

    even = 1 - lax.rem(me, 2)
    across = 1 - even
    closing = one_round and devices >= 4
    first, last = me == 0, me == devices - 1
    gives, takes, feeds = first, last, me == 1

    barrier = pltpu.get_barrier_semaphore()
    partners = far_partners + near_partners
    if not one_round:
        partners = [ring(0), ring(1)] + partners
    for partner in partners:
        pl.semaphore_signal(barrier, inc=1, device_id=partner, device_id_type=MESH)
    for load in (load_guess, load_cols, load_values, load_rhs):
        load.start()


    def send(step, source, way):
        return pltpu.make_async_remote_copy(
            src_ref=source,
            dst_ref=beside.at[step, way],
            send_sem=cross_sem.at[0] if way is even else chip_sem.at[0],
            recv_sem=(
                cross_sem.at[1] if way is even else chip_sem.at[1 + lax.rem(step, 2)]
            ),
            device_id=ring(way),
            device_id_type=MESH,
        )


    def over(source, target, i):
        return pltpu.make_async_remote_copy(
            src_ref=source,
            dst_ref=target,
            send_sem=ghost_sem.at[2 * i],
            recv_sem=ghost_sem.at[2 * i + 1],
            device_id=ring(even),
            device_id_type=MESH,
        )

    def give():
        k = 1 + across
        piece = pl.ds(k * per_block, per_block)
        return [
            over(values.at[piece], ghost_values.at[piece], 0),
            over(local_of.at[k], ghost_local.at[k], 0),
        ]

    def give_rest(i):
        k = 2 - across
        if i == 0:
            tail = pl.ds(3, blocks - 3)
            return [
                over(local_of.at[tail], ghost_local.at[tail], 1),
                over(local_of.at[k], ghost_local.at[k], 1),
            ]
        block = k if i == 2 else own[max(i - 2, 0)]
        piece = pl.ds(block * per_block, per_block)
        return [over(values.at[piece], ghost_values.at[piece], 1)]

    def given(count, i):
        some = pl.ds(0, count)
        return over(values.at[some], ghost_values.at[some], i)

    block_given = given(per_block + tiles, 0)
    rest_given = given((blocks - 1) * per_block + (blocks - 2) * tiles, 1)

    def give_more(when, *which):
        if closing and which:
            @pl.when(first & when)
            def _():
                for i in which:
                    for copy in give_rest(i):
                        copy.start()

    def feed(t):
        to = jnp.where(me == 1, devices - 1, 0)
        return pltpu.make_async_remote_copy(
            src_ref=field.at[t],
            dst_ref=beyond.at[t],
            send_sem=ghost_sem.at[4],
            recv_sem=ghost_sem.at[5],
            device_id=(to // aggs, lax.rem(to, aggs)),
            device_id_type=MESH,
        )

    def give_part(t):
        return pltpu.make_async_remote_copy(
            src_ref=part.at[t],
            dst_ref=ghost_part.at[t],
            send_sem=cross_sem.at[0],
            recv_sem=cross_sem.at[2 + t],
            device_id=ring(even),
            device_id_type=MESH,
        )

    low = jnp.full((tiles, LANES), low_ref[0], jnp.int32).astype(jnp.float32) / 4.0
    high = jnp.full((tiles, LANES), high_ref[0], jnp.int32).astype(jnp.float32) / 4.0
    centre = (high + low) / 2.0
    half = (high - low) / 2.0
    spread = centre / half
    ratio = 1.0 / spread
    coef[0, 0] = jnp.zeros((tiles, LANES), jnp.float32)
    coef[0, 1] = 1.0 / centre
    for t in range(1, STEPS):
        ahead = 1.0 / (2.0 * spread - ratio)
        coef[t, 0] = ahead * ratio
        coef[t, 1] = 2.0 * ahead / half
        ratio = ahead

    load_cols.wait()
    for c in range(tiles):
        cols_flat[pl.ds(c * 8, blocks), :] = cols[:, c * LANES:(c + 1) * LANES]
    for k in range(1, blocks):
        plane = {1: previous, 2: following}.get(k, me)
        local_of[k] = cols_flat[pl.ds(k, tiles, stride=8), :] - plane * rows

    def taken(source, local):
        lanes, tile = local & (LANES - 1), local >> 7
        out = [None] * comp
        for r in range(tiles):
            here = tile == r
            for j in range(comp):
                row = jnp.broadcast_to(source[pl.ds(r * comp + j, 1), :], (tiles, LANES))
                got = gather_lanes(row, lanes)
                out[j] = got if r == 0 else jnp.where(here, got, out[j])
        return out

    def combine(k, got, total, values=values):
        total = list(total)
        for i in range(comp):
            base = (k * comp + i) * comp * tiles
            for j in range(comp):
                total[i] = total[i] - values[pl.ds(base + j, tiles, stride=comp), :] * got[j]
        return total

    def own_part(t, residual):
        source = field.at[t]
        direct = [source[pl.ds(j, tiles, stride=comp), :] for j in range(comp)]
        residual = combine(0, direct, residual)
        for k in own[1:]:
            residual = combine(k, taken(source, local_of[k]), residual)
        return direct, residual

    def far_part(t, way, residual):
        k = 1 + way
        return combine(k, taken(beside.at[t, way], local_of[k]), residual)

    def arrive(t, way):
        send(t, field.at[t], across if way is even else even).wait_recv()

    def advance(t, direct, residual):
        for j in range(comp):
            field[t + 1, pl.ds(j, tiles, stride=comp), :] = (
                coef[t, 0] * direct[j] + coef[t, 1] * residual[j]
            )

    load_guess.wait()
    pl.semaphore_wait(barrier, len(partners))
    for way in (even, across):
        send(0, field.at[0], way).start()
    load_values.wait()
    for copy in give():
        copy.start()
    load_rhs.wait()

    def foresee(t, total):
        source = beside.at[t, across]
        for j in range(comp):
            ghost_residual[pl.ds(j, tiles, stride=comp), :] = total[j]
            beside[t + 1, across, pl.ds(j, tiles, stride=comp), :] = (
                coef[t, 0] * source[pl.ds(j, tiles, stride=comp), :] + coef[t, 1] * total[j]
            )

    def foresee_alone(t):
        source = beside.at[t, across]
        total = [ghost_residual[pl.ds(j, tiles, stride=comp), :] for j in range(comp)]
        direct = [source[pl.ds(j, tiles, stride=comp), :] for j in range(comp)]
        total = combine(0, direct, total, ghost_values)
        for k in own[1:]:
            total = combine(k, taken(source, ghost_local[k]), total, ghost_values)
        k = 2 - across
        total = combine(k, taken(field.at[t], ghost_local[k]), total, ghost_values)
        feed(t).wait_recv()
        k = 1 + across
        total = combine(k, taken(beyond.at[t], ghost_local[k]), total, ghost_values)
        foresee(t, total)

    def foresee_from(t):
        give_part(t).wait_recv()
        other = [ghost_part[t, pl.ds(j, tiles, stride=comp), :] for j in range(comp)]
        k = 2 - across
        foresee(t, combine(k, taken(field.at[t], ghost_local[k]), other, ghost_values))

    def step(t, carry):
        smoothed, residual = carry
        direct, residual = own_part(t, residual)
        smoothed = [s + d for s, d in zip(smoothed, direct)]
        arrive(t, even)
        residual = far_part(t, even, residual)

        @pl.when(jnp.logical_not(first & (t == STEPS - 1)) if closing else True)
        def _():
            for j in range(comp):
                part[t, pl.ds(j, tiles, stride=comp), :] = residual[j]
            give_part(t).start()
        give_more(t == 0, 0, 1)
        give_more(t == 2, 5, 6)

        @pl.when(t == 0)
        def _():
            arrive(0, across)

        @pl.when(t == 1)
        def _():
            block_given.wait_recv()

        @pl.when(t > 0)
        def _():
            foresee_from(t - 1)
        residual = far_part(t, across, residual)
        advance(t, direct, residual)
        send(t + 1, field.at[t + 1], across).start()
        if closing:
            @pl.when(feeds & (t == STEPS - 2))
            def _():
                feed(t + 1).start()
        give_more(t == 0, 2)
        give_more(t == 1, 3, 4)
        return smoothed, residual

    smoothed = [jnp.zeros((tiles, LANES), jnp.float32) for j in range(comp)]
    residual = [rhs[pl.ds(j, tiles, stride=comp), :] for j in range(comp)]
    smoothed, residual = lax.fori_loop(0, STEPS, step, (smoothed, residual))

    direct, residual = own_part(STEPS, residual)
    for j in range(comp):
        smoothed_out[pl.ds(j, tiles, stride=comp), :] = smoothed[j] + direct[j]
    arrive(STEPS, even)
    residual = far_part(STEPS, even, residual)

    @pl.when(jnp.logical_not(takes) if closing else True)
    def _():
        foresee_from(STEPS - 1)
    if closing:
        @pl.when(takes)
        def _():
            rest_given.wait_recv()
            foresee_alone(STEPS - 1)
    residual = far_part(STEPS, across, residual)

    squares = residual[0] * residual[0]
    for j in range(1, comp):
        squares = squares + residual[j] * residual[j]
    partial = jnp.sum(squares, axis=0, keepdims=True)

    def spread_sums(sums, slot, partner, sems):
        return pltpu.make_async_remote_copy(
            src_ref=sums.at[slot],
            dst_ref=sums.at[slot],
            send_sem=sems.at[0],
            recv_sem=sems.at[1],
            device_id=partner,
            device_id_type=MESH,
        )

    def sent(count, way):
        planes = pl.ds(0, count)
        return pltpu.make_async_remote_copy(
            src_ref=field.at[planes],
            dst_ref=beyond.at[planes],
            send_sem=cross_sem.at[0] if way is even else chip_sem.at[0],
            recv_sem=ghost_sem.at[5],
            device_id=ring(way),
            device_id_type=MESH,
        )

    def wait_sends():
        sent(STEPS + 1, across).wait_send()
        block_given.wait_send()

        @pl.when(jnp.logical_not(gives) if closing else True)
        def _():
            sent(STEPS + 1, even).wait_send()
        if closing:
            @pl.when(gives)
            def _():
                sent(STEPS, even).wait_send()
                rest_given.wait_send()

            @pl.when(feeds)
            def _():
                feed(STEPS - 1).wait_send()

    near_sums[near_me] = partial
    for partner in near_partners:
        spread_sums(near_sums, near_me, partner, sum_sem.at[pl.ds(0, 2)]).start()
    for j in range(comp):
        residual_out[pl.ds(j, tiles, stride=comp), :] = residual[j]
    wait_sends()
    if near_partners:
        every_near = pl.ds(0, len(near_partners))
        spread_sums(near_sums, every_near, near_partners[0], sum_sem.at[pl.ds(0, 2)]).wait_recv()
    total = jnp.sum(near_sums[...], axis=0)
    if far_partners:
        far_sums[sub] = total
        for partner in far_partners:
            spread_sums(far_sums, sub, partner, sum_sem.at[pl.ds(2, 2)]).start()
        every = pl.ds(0, len(far_partners))
        spread_sums(far_sums, every, far_partners[0], sum_sem.at[pl.ds(2, 2)]).wait_send()
        spread_sums(far_sums, every, far_partners[0], sum_sem.at[pl.ds(2, 2)]).wait_recv()
        total = jnp.sum(far_sums[...], axis=0)
    count = float(comp * rows * devices)
    rms_ref[...] = jnp.broadcast_to(jnp.sqrt(jnp.sum(total, axis=1, keepdims=True) / count + 1e-06), rms_ref.shape)
    if near_partners:
        spread_sums(near_sums, every_near, near_partners[0], sum_sem.at[pl.ds(0, 2)]).wait_send()


def put_out(*refs):
    count = len(refs) // 2
    sems = refs[-1]
    copies = [
        pltpu.make_async_copy(refs[i] if i < 2 else refs[i].at[pl.ds(0, 1)], refs[count + i], sems.at[i]) for i in range(count)
    ]
    for copy in copies:
        copy.start()
    for copy in copies:
        copy.wait()


def flat(field, tiles):
    comp = field.shape[-2]
    lead = field.shape[:-2]
    cut = field.reshape(lead + (comp, tiles, LANES))
    return jnp.swapaxes(cut, -3, -2).reshape(-1, LANES)


def unflat(field, comp):
    tiles = field.shape[0] // comp
    return jnp.swapaxes(field.reshape(tiles, comp, LANES), 0, 1).reshape(comp, tiles * LANES)


def shards(subs, aggs, block_values, block_cols, coarse_rhs, guess, bound_low, bound_high):
    blocks, comp, _, rows = block_values.shape
    tiles = rows // LANES
    devices = subs * aggs
    near, far = (devices, 1) if devices <= ONE_ROUND else (aggs, subs)
    f32 = jnp.float32
    plane = (tiles * comp, LANES)
    anywhere = pl.BlockSpec(memory_space=pl.ANY)
    in_vmem = pl.BlockSpec(memory_space=pltpu.VMEM)
    in_hbm = pl.BlockSpec(memory_space=pltpu.HBM)
    dma = pltpu.SemaphoreType.DMA
    smoothed, residual, rms = pl.pallas_call(
        functools.partial(kernel, subs, aggs, (blocks, comp, tiles)),
        out_shape=(
            jax.ShapeDtypeStruct(plane, f32),
            jax.ShapeDtypeStruct(plane, f32),
            jax.ShapeDtypeStruct((8, LANES), f32),
        ),
        in_specs=[in_hbm] * 4 + [pl.BlockSpec(memory_space=pltpu.SMEM)] * 2,
        out_specs=(in_vmem,) * 3,
        scratch_shapes=[
            pltpu.VMEM((blocks * comp * comp * tiles, LANES), f32),
            pltpu.VMEM((blocks, rows), jnp.int32),
            pltpu.VMEM((8 * tiles, LANES), jnp.int32),
            pltpu.VMEM(plane, f32),
            pltpu.VMEM((STEPS + 1,) + plane, f32),
            pltpu.VMEM((STEPS + 1, 2) + plane, f32),
            pltpu.VMEM((blocks, tiles, LANES), jnp.int32),
            pltpu.VMEM((STEPS, 2, tiles, LANES), f32),
            pltpu.VMEM((near, 1, LANES), f32),
            pltpu.VMEM((far, 1, LANES), f32),
            pltpu.VMEM((blocks * comp * comp * tiles, LANES), f32),
            pltpu.VMEM((blocks, tiles, LANES), jnp.int32),
            pltpu.VMEM(plane, f32),
            pltpu.VMEM((STEPS + 1,) + plane, f32),
            pltpu.VMEM((STEPS,) + plane, f32),
            pltpu.VMEM((STEPS,) + plane, f32),
            dma((4,)),
            dma((3,)),
            dma((2 + STEPS,)),
            dma((6,)),
            dma((2 if far == 1 else 4,)),
        ],
        compiler_params=pltpu.CompilerParams(collective_id=0, has_side_effects=True, vmem_limit_bytes=8 * 1024 * 1024),
    )(
        *[
            pltpu.with_memory_space_constraint(x, pltpu.HBM)
            for x in (
                flat(block_values, tiles), block_cols, flat(coarse_rhs, tiles), flat(guess, tiles),
            )
        ],
        bound_low, bound_high,
    )
    smoothed, residual, rms = pl.pallas_call(
        put_out,
        out_shape=(
            jax.ShapeDtypeStruct(plane, f32),
            jax.ShapeDtypeStruct(plane, f32),
            jax.ShapeDtypeStruct((1, LANES), f32),
        ),
        in_specs=[anywhere] * 3,
        out_specs=(anywhere,) * 3,
        scratch_shapes=[dma((3,))],
        compiler_params=pltpu.CompilerParams(vmem_limit_bytes=8 * 1024 * 1024),
    )(smoothed, residual, rms)
    return unflat(smoothed, comp), unflat(residual, comp), rms[0,:1]


def solution(mesh):
    split = ("sub", "agg")
    return jax.shard_map(
        functools.partial(shards, mesh.shape["sub"], mesh.shape["agg"]),
        mesh=mesh,
        in_specs=(
            P(None, None, None, split),
            P(None, split),
            P(None, split),
            P(None, split),
            P(),
            P(),
        ),
        out_specs=(P(None, split), P(None, split), P()),
        check_vma=False,
    )
```

```python
import functools

import jax
import jax.numpy as jnp
from jax import lax
from jax.experimental import pallas as pl
from jax.experimental.pallas import tpu as pltpu
from jax.sharding import PartitionSpec as P

STEPS = 4
ONE_ROUND = 32
LANES = 128
MESH = pl.DeviceIdType.MESH


def gather_lanes(rows, index):
    return jnp.take_along_axis(rows, index, axis=1, mode="promise_in_bounds")


def kernel(
    subs, aggs, shape,
    values_hbm, cols_hbm, rhs_hbm, guess_hbm, low_ref, high_ref,
    smoothed_out, residual_out, rms_ref,
    values, cols, cols_flat, rhs, field, beside, local_of, coef,
    near_sums, far_sums,
    ghost_values, ghost_local, ghost_residual, beyond, part, ghost_part,
    load_sem, chip_sem, cross_sem, ghost_sem, sum_sem,
):
    blocks, comp, tiles = shape
    devices = subs * aggs
    rows = tiles * LANES
    load_cols = pltpu.make_async_copy(cols_hbm, cols, load_sem.at[0])
    load_guess = pltpu.make_async_copy(guess_hbm, field.at[0], load_sem.at[1])
    load_rhs = pltpu.make_async_copy(rhs_hbm, rhs, load_sem.at[3])
    load_values = pltpu.make_async_copy(values_hbm, values, load_sem.at[2])
    own = [0] + list(range(3, blocks))
    per_block = comp * comp * tiles


    sub, agg = lax.axis_index("sub"), lax.axis_index("agg")
    me = sub * aggs + agg

    def ahead_of(place, by, size):
        to = place + by
        return jnp.where(to >= size, to - size, to)

    def beside_me(by_sub, by_agg):
        return (ahead_of(sub, by_sub, subs), ahead_of(agg, by_agg, aggs))

    def ring(way):
        turn = jnp.where(way == 0, agg == aggs - 1, agg == 0)
        to_sub = jnp.where(way == 0, ahead_of(sub, 1, subs), ahead_of(sub, subs - 1, subs))
        to_agg = jnp.where(way == 0, ahead_of(agg, 1, aggs), ahead_of(agg, aggs - 1, aggs))
        return (jnp.where(turn, to_sub, sub), to_agg)

    following = ahead_of(me, 1, devices)
    previous = ahead_of(me, devices - 1, devices)
    one_round = devices <= ONE_ROUND
    if one_round:
        low = sub < subs // 2
        near_steps = [
            (jnp.where(low, subs - a, a), b) for a in range(1, subs) for b in range(aggs)
        ] + [(0, b) for b in range(1, aggs)]
        near, near_me = devices, me
        far_steps = []
    else:
        near_steps = [(0, b) for b in range(1, aggs)]
        near, near_me = aggs, agg
        far_steps = [(a, 0) for a in range(1, subs)]
    near_partners = [beside_me(a, b) for a, b in near_steps]
    far_partners = [beside_me(a, b) for a, b in far_steps]

    even = 1 - lax.rem(me, 2)
    across = 1 - even
    closing = one_round and devices >= 4
    first, last = me == 0, me == devices - 1
    gives, takes, feeds = first, last, me == 1

    barrier = pltpu.get_barrier_semaphore()
    partners = far_partners + near_partners
    if not one_round:
        partners = [ring(0), ring(1)] + partners
    for partner in partners:
        pl.semaphore_signal(barrier, inc=1, device_id=partner, device_id_type=MESH)
    for load in (load_guess, load_cols, load_values, load_rhs):
        load.start()


    def send(step, source, way):
        return pltpu.make_async_remote_copy(
            src_ref=source,
            dst_ref=beside.at[step, way],
            send_sem=cross_sem.at[0] if way is even else chip_sem.at[0],
            recv_sem=(
                cross_sem.at[1] if way is even else chip_sem.at[1 + lax.rem(step, 2)]
            ),
            device_id=ring(way),
            device_id_type=MESH,
        )


    def over(source, target, i):
        return pltpu.make_async_remote_copy(
            src_ref=source,
            dst_ref=target,
            send_sem=ghost_sem.at[2 * i],
            recv_sem=ghost_sem.at[2 * i + 1],
            device_id=ring(even),
            device_id_type=MESH,
        )

    def give():
        k = 1 + across
        piece = pl.ds(k * per_block, per_block)
        return [
            over(values.at[piece], ghost_values.at[piece], 0),
            over(local_of.at[k], ghost_local.at[k], 0),
        ]

    def give_rest(i):
        k = 2 - across
        if i == 0:
            tail = pl.ds(3, blocks - 3)
            return [
                over(local_of.at[tail], ghost_local.at[tail], 1),
                over(local_of.at[k], ghost_local.at[k], 1),
            ]
        block = k if i == 2 else own[max(i - 2, 0)]
        piece = pl.ds(block * per_block, per_block)
        return [over(values.at[piece], ghost_values.at[piece], 1)]

    def given(count, i):
        some = pl.ds(0, count)
        return over(values.at[some], ghost_values.at[some], i)

    block_given = given(per_block + tiles, 0)
    rest_given = given((blocks - 1) * per_block + (blocks - 2) * tiles, 1)

    def give_more(when, *which):
        if closing and which:
            @pl.when(first & when)
            def _():
                for i in which:
                    for copy in give_rest(i):
                        copy.start()

    def feed(t):
        to = jnp.where(me == 1, devices - 1, 0)
        return pltpu.make_async_remote_copy(
            src_ref=field.at[t],
            dst_ref=beyond.at[t],
            send_sem=ghost_sem.at[4],
            recv_sem=ghost_sem.at[5],
            device_id=(to // aggs, lax.rem(to, aggs)),
            device_id_type=MESH,
        )

    def give_part(t):
        return pltpu.make_async_remote_copy(
            src_ref=part.at[t],
            dst_ref=ghost_part.at[t],
            send_sem=cross_sem.at[0],
            recv_sem=cross_sem.at[2 + t],
            device_id=ring(even),
            device_id_type=MESH,
        )

    low = jnp.full((tiles, LANES), low_ref[0], jnp.int32).astype(jnp.float32) / 4.0
    high = jnp.full((tiles, LANES), high_ref[0], jnp.int32).astype(jnp.float32) / 4.0
    centre = (high + low) / 2.0
    half = (high - low) / 2.0
    spread = centre / half
    ratio = 1.0 / spread
    coef[0, 0] = jnp.zeros((tiles, LANES), jnp.float32)
    coef[0, 1] = 1.0 / centre
    for t in range(1, STEPS):
        ahead = 1.0 / (2.0 * spread - ratio)
        coef[t, 0] = ahead * ratio
        coef[t, 1] = 2.0 * ahead / half
        ratio = ahead

    load_cols.wait()
    for c in range(tiles):
        cols_flat[pl.ds(c * 8, blocks), :] = cols[:, c * LANES:(c + 1) * LANES]
    for k in range(1, blocks):
        plane = {1: previous, 2: following}.get(k, me)
        local_of[k] = cols_flat[pl.ds(k, tiles, stride=8), :] - plane * rows

    def taken(source, local):
        lanes, tile = local & (LANES - 1), local >> 7
        out = [None] * comp
        for r in range(tiles):
            here = tile == r
            for j in range(comp):
                row = jnp.broadcast_to(source[pl.ds(r * comp + j, 1), :], (tiles, LANES))
                got = gather_lanes(row, lanes)
                out[j] = got if r == 0 else jnp.where(here, got, out[j])
        return out

    def combine(k, got, total, values=values):
        total = list(total)
        for i in range(comp):
            base = (k * comp + i) * comp * tiles
            for j in range(comp):
                total[i] = total[i] - values[pl.ds(base + j, tiles, stride=comp), :] * got[j]
        return total

    def own_part(t, residual):
        source = field.at[t]
        direct = [source[pl.ds(j, tiles, stride=comp), :] for j in range(comp)]
        residual = combine(0, direct, residual)
        for k in own[1:]:
            residual = combine(k, taken(source, local_of[k]), residual)
        return direct, residual

    def far_part(t, way, residual):
        k = 1 + way
        return combine(k, taken(beside.at[t, way], local_of[k]), residual)

    def arrive(t, way):
        send(t, field.at[t], across if way is even else even).wait_recv()

    def advance(t, direct, residual):
        for j in range(comp):
            field[t + 1, pl.ds(j, tiles, stride=comp), :] = (
                coef[t, 0] * direct[j] + coef[t, 1] * residual[j]
            )

    load_guess.wait()
    pl.semaphore_wait(barrier, len(partners))
    for way in (even, across):
        send(0, field.at[0], way).start()
    load_values.wait()
    for copy in give():
        copy.start()
    load_rhs.wait()

    def foresee(t, total):
        source = beside.at[t, across]
        for j in range(comp):
            ghost_residual[pl.ds(j, tiles, stride=comp), :] = total[j]
            beside[t + 1, across, pl.ds(j, tiles, stride=comp), :] = (
                coef[t, 0] * source[pl.ds(j, tiles, stride=comp), :] + coef[t, 1] * total[j]
            )

    def foresee_alone(t):
        source = beside.at[t, across]
        total = [ghost_residual[pl.ds(j, tiles, stride=comp), :] for j in range(comp)]
        direct = [source[pl.ds(j, tiles, stride=comp), :] for j in range(comp)]
        total = combine(0, direct, total, ghost_values)
        for k in own[1:]:
            total = combine(k, taken(source, ghost_local[k]), total, ghost_values)
        k = 2 - across
        total = combine(k, taken(field.at[t], ghost_local[k]), total, ghost_values)
        feed(t).wait_recv()
        k = 1 + across
        total = combine(k, taken(beyond.at[t], ghost_local[k]), total, ghost_values)
        foresee(t, total)

    def foresee_from(t):
        k = 2 - across
        mine = [jnp.zeros((tiles, LANES), jnp.float32) for j in range(comp)]
        mine = combine(k, taken(field.at[t], ghost_local[k]), mine, ghost_values)
        give_part(t).wait_recv()
        foresee(t, [ghost_part[t, pl.ds(j, tiles, stride=comp), :] + mine[j] for j in range(comp)])

    def step(t, carry):
        smoothed, residual = carry
        direct, residual = own_part(t, residual)
        smoothed = [s + d for s, d in zip(smoothed, direct)]
        arrive(t, even)
        residual = far_part(t, even, residual)

        @pl.when(jnp.logical_not(first & (t == STEPS - 1)) if closing else True)
        def _():
            for j in range(comp):
                part[t, pl.ds(j, tiles, stride=comp), :] = residual[j]
            give_part(t).start()
        give_more(t == 0, 0, 1)
        give_more(t == 2, 5, 6)

        @pl.when(t == 0)
        def _():
            arrive(0, across)

        @pl.when(t == 1)
        def _():
            block_given.wait_recv()

        @pl.when(t > 0)
        def _():
            foresee_from(t - 1)
        residual = far_part(t, across, residual)
        advance(t, direct, residual)
        send(t + 1, field.at[t + 1], across).start()
        if closing:
            @pl.when(feeds & (t == STEPS - 2))
            def _():
                feed(t + 1).start()
        give_more(t == 0, 2)
        give_more(t == 1, 3, 4)
        return smoothed, residual

    smoothed = [jnp.zeros((tiles, LANES), jnp.float32) for j in range(comp)]
    residual = [rhs[pl.ds(j, tiles, stride=comp), :] for j in range(comp)]
    smoothed, residual = lax.fori_loop(0, STEPS, step, (smoothed, residual))

    direct, residual = own_part(STEPS, residual)
    for j in range(comp):
        smoothed_out[pl.ds(j, tiles, stride=comp), :] = smoothed[j] + direct[j]
    arrive(STEPS, even)
    residual = far_part(STEPS, even, residual)

    @pl.when(jnp.logical_not(takes) if closing else True)
    def _():
        foresee_from(STEPS - 1)
    if closing:
        @pl.when(takes)
        def _():
            rest_given.wait_recv()
            foresee_alone(STEPS - 1)
    residual = far_part(STEPS, across, residual)

    squares = residual[0] * residual[0]
    for j in range(1, comp):
        squares = squares + residual[j] * residual[j]
    partial = jnp.sum(squares, axis=0, keepdims=True)

    def spread_sums(sums, slot, partner, sems):
        return pltpu.make_async_remote_copy(
            src_ref=sums.at[slot],
            dst_ref=sums.at[slot],
            send_sem=sems.at[0],
            recv_sem=sems.at[1],
            device_id=partner,
            device_id_type=MESH,
        )

    def sent(count, way):
        planes = pl.ds(0, count)
        return pltpu.make_async_remote_copy(
            src_ref=field.at[planes],
            dst_ref=beyond.at[planes],
            send_sem=cross_sem.at[0] if way is even else chip_sem.at[0],
            recv_sem=ghost_sem.at[5],
            device_id=ring(way),
            device_id_type=MESH,
        )

    def wait_sends():
        sent(STEPS + 1, across).wait_send()
        block_given.wait_send()

        @pl.when(jnp.logical_not(gives) if closing else True)
        def _():
            sent(STEPS + 1, even).wait_send()
        if closing:
            @pl.when(gives)
            def _():
                sent(STEPS, even).wait_send()
                rest_given.wait_send()

            @pl.when(feeds)
            def _():
                feed(STEPS - 1).wait_send()

    near_sums[near_me] = partial
    for partner in near_partners:
        spread_sums(near_sums, near_me, partner, sum_sem.at[pl.ds(0, 2)]).start()
    for j in range(comp):
        residual_out[pl.ds(j, tiles, stride=comp), :] = residual[j]
    wait_sends()
    if near_partners:
        every_near = pl.ds(0, len(near_partners))
        spread_sums(near_sums, every_near, near_partners[0], sum_sem.at[pl.ds(0, 2)]).wait_recv()
    total = jnp.sum(near_sums[...], axis=0)
    if far_partners:
        far_sums[sub] = total
        for partner in far_partners:
            spread_sums(far_sums, sub, partner, sum_sem.at[pl.ds(2, 2)]).start()
        every = pl.ds(0, len(far_partners))
        spread_sums(far_sums, every, far_partners[0], sum_sem.at[pl.ds(2, 2)]).wait_send()
        spread_sums(far_sums, every, far_partners[0], sum_sem.at[pl.ds(2, 2)]).wait_recv()
        total = jnp.sum(far_sums[...], axis=0)
    count = float(comp * rows * devices)
    rms_ref[...] = jnp.broadcast_to(jnp.sqrt(jnp.sum(total, axis=1, keepdims=True) / count + 1e-06), rms_ref.shape)
    if near_partners:
        spread_sums(near_sums, every_near, near_partners[0], sum_sem.at[pl.ds(0, 2)]).wait_send()


def put_out(*refs):
    count = len(refs) // 2
    sems = refs[-1]
    copies = [
        pltpu.make_async_copy(refs[i] if i < 2 else refs[i].at[pl.ds(0, 1)], refs[count + i], sems.at[i]) for i in range(count)
    ]
    for copy in copies:
        copy.start()
    for copy in copies:
        copy.wait()


def flat(field, tiles):
    comp = field.shape[-2]
    lead = field.shape[:-2]
    cut = field.reshape(lead + (comp, tiles, LANES))
    return jnp.swapaxes(cut, -3, -2).reshape(-1, LANES)


def unflat(field, comp):
    tiles = field.shape[0] // comp
    return jnp.swapaxes(field.reshape(tiles, comp, LANES), 0, 1).reshape(comp, tiles * LANES)


def shards(subs, aggs, block_values, block_cols, coarse_rhs, guess, bound_low, bound_high):
    blocks, comp, _, rows = block_values.shape
    tiles = rows // LANES
    devices = subs * aggs
    near, far = (devices, 1) if devices <= ONE_ROUND else (aggs, subs)
    f32 = jnp.float32
    plane = (tiles * comp, LANES)
    anywhere = pl.BlockSpec(memory_space=pl.ANY)
    in_vmem = pl.BlockSpec(memory_space=pltpu.VMEM)
    in_hbm = pl.BlockSpec(memory_space=pltpu.HBM)
    dma = pltpu.SemaphoreType.DMA
    smoothed, residual, rms = pl.pallas_call(
        functools.partial(kernel, subs, aggs, (blocks, comp, tiles)),
        out_shape=(
            jax.ShapeDtypeStruct(plane, f32),
            jax.ShapeDtypeStruct(plane, f32),
            jax.ShapeDtypeStruct((8, LANES), f32),
        ),
        in_specs=[in_hbm] * 4 + [pl.BlockSpec(memory_space=pltpu.SMEM)] * 2,
        out_specs=(in_vmem,) * 3,
        scratch_shapes=[
            pltpu.VMEM((blocks * comp * comp * tiles, LANES), f32),
            pltpu.VMEM((blocks, rows), jnp.int32),
            pltpu.VMEM((8 * tiles, LANES), jnp.int32),
            pltpu.VMEM(plane, f32),
            pltpu.VMEM((STEPS + 1,) + plane, f32),
            pltpu.VMEM((STEPS + 1, 2) + plane, f32),
            pltpu.VMEM((blocks, tiles, LANES), jnp.int32),
            pltpu.VMEM((STEPS, 2, tiles, LANES), f32),
            pltpu.VMEM((near, 1, LANES), f32),
            pltpu.VMEM((far, 1, LANES), f32),
            pltpu.VMEM((blocks * comp * comp * tiles, LANES), f32),
            pltpu.VMEM((blocks, tiles, LANES), jnp.int32),
            pltpu.VMEM(plane, f32),
            pltpu.VMEM((STEPS + 1,) + plane, f32),
            pltpu.VMEM((STEPS,) + plane, f32),
            pltpu.VMEM((STEPS,) + plane, f32),
            dma((4,)),
            dma((3,)),
            dma((2 + STEPS,)),
            dma((6,)),
            dma((2 if far == 1 else 4,)),
        ],
        compiler_params=pltpu.CompilerParams(collective_id=0, has_side_effects=True, vmem_limit_bytes=8 * 1024 * 1024),
    )(
        *[
            pltpu.with_memory_space_constraint(x, pltpu.HBM)
            for x in (
                flat(block_values, tiles), block_cols, flat(coarse_rhs, tiles), flat(guess, tiles),
            )
        ],
        bound_low, bound_high,
    )
    smoothed, residual, rms = pl.pallas_call(
        put_out,
        out_shape=(
            jax.ShapeDtypeStruct(plane, f32),
            jax.ShapeDtypeStruct(plane, f32),
            jax.ShapeDtypeStruct((1, LANES), f32),
        ),
        in_specs=[anywhere] * 3,
        out_specs=(anywhere,) * 3,
        scratch_shapes=[dma((3,))],
        compiler_params=pltpu.CompilerParams(vmem_limit_bytes=8 * 1024 * 1024),
    )(smoothed, residual, rms)
    return unflat(smoothed, comp), unflat(residual, comp), rms[0,:1]


def solution(mesh):
    split = ("sub", "agg")
    return jax.shard_map(
        functools.partial(shards, mesh.shape["sub"], mesh.shape["agg"]),
        mesh=mesh,
        in_specs=(
            P(None, None, None, split),
            P(None, split),
            P(None, split),
            P(None, split),
            P(),
            P(),
        ),
        out_specs=(P(None, split), P(None, split), P()),
        check_vma=False,
    )
```

```python
import functools

import jax
import jax.numpy as jnp
from jax import lax
from jax.experimental import pallas as pl
from jax.experimental.pallas import tpu as pltpu
from jax.sharding import PartitionSpec as P

STEPS = 4
ONE_ROUND = 32
LANES = 128
MESH = pl.DeviceIdType.MESH


def gather_lanes(rows, index):
    return jnp.take_along_axis(rows, index, axis=1, mode="promise_in_bounds")


def kernel(
    subs, aggs, shape,
    values_hbm, cols_hbm, rhs_hbm, guess_hbm, low_ref, high_ref,
    smoothed_out, residual_out, rms_ref,
    values, cols, cols_flat, rhs, field, beside, local_of, coef,
    near_sums, far_sums,
    ghost_values, ghost_local, ghost_residual, beyond, part, ghost_part,
    load_sem, chip_sem, cross_sem, ghost_sem, sum_sem,
):
    blocks, comp, tiles = shape
    devices = subs * aggs
    rows = tiles * LANES
    load_cols = pltpu.make_async_copy(cols_hbm, cols, load_sem.at[0])
    load_guess = pltpu.make_async_copy(guess_hbm, field.at[0], load_sem.at[1])
    load_rhs = pltpu.make_async_copy(rhs_hbm, rhs, load_sem.at[3])
    load_values = pltpu.make_async_copy(values_hbm, values, load_sem.at[2])
    own = [0] + list(range(3, blocks))
    per_block = comp * comp * tiles


    sub, agg = lax.axis_index("sub"), lax.axis_index("agg")
    me = sub * aggs + agg

    def ahead_of(place, by, size):
        to = place + by
        return jnp.where(to >= size, to - size, to)

    def beside_me(by_sub, by_agg):
        return (ahead_of(sub, by_sub, subs), ahead_of(agg, by_agg, aggs))

    def ring(way):
        turn = jnp.where(way == 0, agg == aggs - 1, agg == 0)
        to_sub = jnp.where(way == 0, ahead_of(sub, 1, subs), ahead_of(sub, subs - 1, subs))
        to_agg = jnp.where(way == 0, ahead_of(agg, 1, aggs), ahead_of(agg, aggs - 1, aggs))
        return (jnp.where(turn, to_sub, sub), to_agg)

    following = ahead_of(me, 1, devices)
    previous = ahead_of(me, devices - 1, devices)
    one_round = devices <= ONE_ROUND
    if one_round:
        low = sub < subs // 2
        near_steps = [
            (jnp.where(low, subs - a, a), b) for a in range(1, subs) for b in range(aggs)
        ] + [(0, b) for b in range(1, aggs)]
        near, near_me = devices, me
        far_steps = []
    else:
        near_steps = [(0, b) for b in range(1, aggs)]
        near, near_me = aggs, agg
        far_steps = [(a, 0) for a in range(1, subs)]
    near_partners = [beside_me(a, b) for a, b in near_steps]
    far_partners = [beside_me(a, b) for a, b in far_steps]

    even = 1 - lax.rem(me, 2)
    across = 1 - even
    closing = one_round and devices >= 4
    first, last = me == 0, me == devices - 1
    gives, takes, feeds = first, last, me == 1

    barrier = pltpu.get_barrier_semaphore()
    partners = far_partners + near_partners
    if not one_round:
        partners = [ring(0), ring(1)] + partners
    for partner in partners:
        pl.semaphore_signal(barrier, inc=1, device_id=partner, device_id_type=MESH)
    for load in (load_guess, load_cols, load_values, load_rhs):
        load.start()


    def send(step, source, way):
        return pltpu.make_async_remote_copy(
            src_ref=source,
            dst_ref=beside.at[step, way],
            send_sem=cross_sem.at[0] if way is even else chip_sem.at[0],
            recv_sem=(
                cross_sem.at[1] if way is even else chip_sem.at[1 + lax.rem(step, 2)]
            ),
            device_id=ring(way),
            device_id_type=MESH,
        )


    def over(source, target, i):
        return pltpu.make_async_remote_copy(
            src_ref=source,
            dst_ref=target,
            send_sem=ghost_sem.at[2 * i],
            recv_sem=ghost_sem.at[2 * i + 1],
            device_id=ring(even),
            device_id_type=MESH,
        )

    def give():
        k = 1 + across
        piece = pl.ds(k * per_block, per_block)
        return [
            over(values.at[piece], ghost_values.at[piece], 0),
            over(local_of.at[k], ghost_local.at[k], 0),
        ]

    def give_rest(i):
        k = 2 - across
        if i == 0:
            tail = pl.ds(3, blocks - 3)
            return [
                over(local_of.at[tail], ghost_local.at[tail], 1),
                over(local_of.at[k], ghost_local.at[k], 1),
            ]
        block = k if i == 2 else own[max(i - 2, 0)]
        piece = pl.ds(block * per_block, per_block)
        return [over(values.at[piece], ghost_values.at[piece], 1)]

    def given(count, i):
        some = pl.ds(0, count)
        return over(values.at[some], ghost_values.at[some], i)

    block_given = given(per_block + tiles, 0)
    rest_given = given((blocks - 1) * per_block + (blocks - 2) * tiles, 1)

    def give_more(when, *which):
        if closing and which:
            @pl.when(first & when)
            def _():
                for i in which:
                    for copy in give_rest(i):
                        copy.start()

    def feed(t):
        to = jnp.where(me == 1, devices - 1, 0)
        return pltpu.make_async_remote_copy(
            src_ref=field.at[t],
            dst_ref=beyond.at[t],
            send_sem=ghost_sem.at[4],
            recv_sem=ghost_sem.at[5],
            device_id=(to // aggs, lax.rem(to, aggs)),
            device_id_type=MESH,
        )

    def give_part(t):
        return pltpu.make_async_remote_copy(
            src_ref=part.at[t],
            dst_ref=ghost_part.at[t],
            send_sem=cross_sem.at[0],
            recv_sem=cross_sem.at[2 + t],
            device_id=ring(even),
            device_id_type=MESH,
        )

    low = jnp.full((tiles, LANES), low_ref[0], jnp.int32).astype(jnp.float32) / 4.0
    high = jnp.full((tiles, LANES), high_ref[0], jnp.int32).astype(jnp.float32) / 4.0
    centre = (high + low) / 2.0
    half = (high - low) / 2.0
    spread = centre / half
    ratio = 1.0 / spread
    coef[0, 0] = jnp.zeros((tiles, LANES), jnp.float32)
    coef[0, 1] = 1.0 / centre
    for t in range(1, STEPS):
        ahead = 1.0 / (2.0 * spread - ratio)
        coef[t, 0] = ahead * ratio
        coef[t, 1] = 2.0 * ahead / half
        ratio = ahead

    load_cols.wait()
    for c in range(tiles):
        cols_flat[pl.ds(c * 8, blocks), :] = cols[:, c * LANES:(c + 1) * LANES]
    for k in range(1, blocks):
        plane = {1: previous, 2: following}.get(k, me)
        local_of[k] = cols_flat[pl.ds(k, tiles, stride=8), :] - plane * rows

    def taken(source, local):
        lanes, tile = local & (LANES - 1), local >> 7
        out = [None] * comp
        for r in range(tiles):
            here = tile == r
            for j in range(comp):
                row = jnp.broadcast_to(source[pl.ds(r * comp + j, 1), :], (tiles, LANES))
                got = gather_lanes(row, lanes)
                out[j] = got if r == 0 else jnp.where(here, got, out[j])
        return out

    def combine(k, got, total, values=values):
        total = list(total)
        for i in range(comp):
            base = (k * comp + i) * comp * tiles
            for j in range(comp):
                total[i] = total[i] - values[pl.ds(base + j, tiles, stride=comp), :] * got[j]
        return total

    def own_part(t, residual):
        source = field.at[t]
        direct = [source[pl.ds(j, tiles, stride=comp), :] for j in range(comp)]
        residual = combine(0, direct, residual)
        for k in own[1:]:
            residual = combine(k, taken(source, local_of[k]), residual)
        return direct, residual

    def far_part(t, way, residual):
        k = 1 + way
        return combine(k, taken(beside.at[t, way], local_of[k]), residual)

    def arrive(t, way):
        send(t, field.at[t], across if way is even else even).wait_recv()

    def advance(t, direct, residual):
        for j in range(comp):
            field[t + 1, pl.ds(j, tiles, stride=comp), :] = (
                coef[t, 0] * direct[j] + coef[t, 1] * residual[j]
            )

    load_guess.wait()
    pl.semaphore_wait(barrier, len(partners))
    for way in (even, across):
        send(0, field.at[0], way).start()
    load_values.wait()
    for copy in give():
        copy.start()
    load_rhs.wait()

    def foresee(t, total):
        source = beside.at[t, across]
        for j in range(comp):
            ghost_residual[pl.ds(j, tiles, stride=comp), :] = total[j]
            beside[t + 1, across, pl.ds(j, tiles, stride=comp), :] = (
                coef[t, 0] * source[pl.ds(j, tiles, stride=comp), :] + coef[t, 1] * total[j]
            )

    def foresee_alone(t):
        source = beside.at[t, across]
        total = [ghost_residual[pl.ds(j, tiles, stride=comp), :] for j in range(comp)]
        direct = [source[pl.ds(j, tiles, stride=comp), :] for j in range(comp)]
        total = combine(0, direct, total, ghost_values)
        for k in own[1:]:
            total = combine(k, taken(source, ghost_local[k]), total, ghost_values)
        k = 2 - across
        total = combine(k, taken(field.at[t], ghost_local[k]), total, ghost_values)
        feed(t).wait_recv()
        k = 1 + across
        total = combine(k, taken(beyond.at[t], ghost_local[k]), total, ghost_values)
        foresee(t, total)

    def foresee_from(t):
        k = 2 - across
        mine = [jnp.zeros((tiles, LANES), jnp.float32) for j in range(comp)]
        mine = combine(k, taken(field.at[t], ghost_local[k]), mine, ghost_values)
        give_part(t).wait_recv()
        foresee(t, [ghost_part[t, pl.ds(j, tiles, stride=comp), :] + mine[j] for j in range(comp)])

    def step(t, carry):
        smoothed, residual = carry
        direct, residual = own_part(t, residual)
        smoothed = [s + d for s, d in zip(smoothed, direct)]
        arrive(t, even)
        residual = far_part(t, even, residual)

        @pl.when(jnp.logical_not(first & (t == STEPS - 1)) if closing else True)
        def _():
            for j in range(comp):
                part[t, pl.ds(j, tiles, stride=comp), :] = residual[j]
            give_part(t).start()
        give_more(t == 0, 0, 1)
        give_more(t == 2, 5, 6)

        @pl.when(t == 0)
        def _():
            arrive(0, across)

        @pl.when(t == 1)
        def _():
            block_given.wait_recv()

        @pl.when(t > 0)
        def _():
            foresee_from(t - 1)
        residual = far_part(t, across, residual)
        advance(t, direct, residual)
        send(t + 1, field.at[t + 1], across).start()
        if closing:
            @pl.when(feeds & (t == STEPS - 2))
            def _():
                feed(t + 1).start()
        give_more(t == 0, 2)
        give_more(t == 1, 3, 4)
        return smoothed, residual

    smoothed = [jnp.zeros((tiles, LANES), jnp.float32) for j in range(comp)]
    residual = [rhs[pl.ds(j, tiles, stride=comp), :] for j in range(comp)]
    smoothed, residual = lax.fori_loop(0, STEPS, step, (smoothed, residual), unroll=True)

    direct, residual = own_part(STEPS, residual)
    for j in range(comp):
        smoothed_out[pl.ds(j, tiles, stride=comp), :] = smoothed[j] + direct[j]
    arrive(STEPS, even)
    residual = far_part(STEPS, even, residual)

    @pl.when(jnp.logical_not(takes) if closing else True)
    def _():
        foresee_from(STEPS - 1)
    if closing:
        @pl.when(takes)
        def _():
            rest_given.wait_recv()
            foresee_alone(STEPS - 1)
    residual = far_part(STEPS, across, residual)

    squares = residual[0] * residual[0]
    for j in range(1, comp):
        squares = squares + residual[j] * residual[j]
    partial = jnp.sum(squares, axis=0, keepdims=True)

    def spread_sums(sums, slot, partner, sems):
        return pltpu.make_async_remote_copy(
            src_ref=sums.at[slot],
            dst_ref=sums.at[slot],
            send_sem=sems.at[0],
            recv_sem=sems.at[1],
            device_id=partner,
            device_id_type=MESH,
        )

    def sent(count, way):
        planes = pl.ds(0, count)
        return pltpu.make_async_remote_copy(
            src_ref=field.at[planes],
            dst_ref=beyond.at[planes],
            send_sem=cross_sem.at[0] if way is even else chip_sem.at[0],
            recv_sem=ghost_sem.at[5],
            device_id=ring(way),
            device_id_type=MESH,
        )

    def wait_sends():
        sent(STEPS + 1, across).wait_send()
        block_given.wait_send()

        @pl.when(jnp.logical_not(gives) if closing else True)
        def _():
            sent(STEPS + 1, even).wait_send()
        if closing:
            @pl.when(gives)
            def _():
                sent(STEPS, even).wait_send()
                rest_given.wait_send()

            @pl.when(feeds)
            def _():
                feed(STEPS - 1).wait_send()

    near_sums[near_me] = partial
    for partner in near_partners:
        spread_sums(near_sums, near_me, partner, sum_sem.at[pl.ds(0, 2)]).start()
    for j in range(comp):
        residual_out[pl.ds(j, tiles, stride=comp), :] = residual[j]
    wait_sends()
    if near_partners:
        every_near = pl.ds(0, len(near_partners))
        spread_sums(near_sums, every_near, near_partners[0], sum_sem.at[pl.ds(0, 2)]).wait_recv()
    total = jnp.sum(near_sums[...], axis=0)
    if far_partners:
        far_sums[sub] = total
        for partner in far_partners:
            spread_sums(far_sums, sub, partner, sum_sem.at[pl.ds(2, 2)]).start()
        every = pl.ds(0, len(far_partners))
        spread_sums(far_sums, every, far_partners[0], sum_sem.at[pl.ds(2, 2)]).wait_send()
        spread_sums(far_sums, every, far_partners[0], sum_sem.at[pl.ds(2, 2)]).wait_recv()
        total = jnp.sum(far_sums[...], axis=0)
    count = float(comp * rows * devices)
    rms_ref[...] = jnp.broadcast_to(jnp.sqrt(jnp.sum(total, axis=1, keepdims=True) / count + 1e-06), rms_ref.shape)
    if near_partners:
        spread_sums(near_sums, every_near, near_partners[0], sum_sem.at[pl.ds(0, 2)]).wait_send()


def put_out(*refs):
    count = len(refs) // 2
    sems = refs[-1]
    copies = [
        pltpu.make_async_copy(refs[i] if i < 2 else refs[i].at[pl.ds(0, 1)], refs[count + i], sems.at[i]) for i in range(count)
    ]
    for copy in copies:
        copy.start()
    for copy in copies:
        copy.wait()


def flat(field, tiles):
    comp = field.shape[-2]
    lead = field.shape[:-2]
    cut = field.reshape(lead + (comp, tiles, LANES))
    return jnp.swapaxes(cut, -3, -2).reshape(-1, LANES)


def unflat(field, comp):
    tiles = field.shape[0] // comp
    return jnp.swapaxes(field.reshape(tiles, comp, LANES), 0, 1).reshape(comp, tiles * LANES)


def shards(subs, aggs, block_values, block_cols, coarse_rhs, guess, bound_low, bound_high):
    blocks, comp, _, rows = block_values.shape
    tiles = rows // LANES
    devices = subs * aggs
    near, far = (devices, 1) if devices <= ONE_ROUND else (aggs, subs)
    f32 = jnp.float32
    plane = (tiles * comp, LANES)
    anywhere = pl.BlockSpec(memory_space=pl.ANY)
    in_vmem = pl.BlockSpec(memory_space=pltpu.VMEM)
    in_hbm = pl.BlockSpec(memory_space=pltpu.HBM)
    dma = pltpu.SemaphoreType.DMA
    smoothed, residual, rms = pl.pallas_call(
        functools.partial(kernel, subs, aggs, (blocks, comp, tiles)),
        out_shape=(
            jax.ShapeDtypeStruct(plane, f32),
            jax.ShapeDtypeStruct(plane, f32),
            jax.ShapeDtypeStruct((8, LANES), f32),
        ),
        in_specs=[in_hbm] * 4 + [pl.BlockSpec(memory_space=pltpu.SMEM)] * 2,
        out_specs=(in_vmem,) * 3,
        scratch_shapes=[
            pltpu.VMEM((blocks * comp * comp * tiles, LANES), f32),
            pltpu.VMEM((blocks, rows), jnp.int32),
            pltpu.VMEM((8 * tiles, LANES), jnp.int32),
            pltpu.VMEM(plane, f32),
            pltpu.VMEM((STEPS + 1,) + plane, f32),
            pltpu.VMEM((STEPS + 1, 2) + plane, f32),
            pltpu.VMEM((blocks, tiles, LANES), jnp.int32),
            pltpu.VMEM((STEPS, 2, tiles, LANES), f32),
            pltpu.VMEM((near, 1, LANES), f32),
            pltpu.VMEM((far, 1, LANES), f32),
            pltpu.VMEM((blocks * comp * comp * tiles, LANES), f32),
            pltpu.VMEM((blocks, tiles, LANES), jnp.int32),
            pltpu.VMEM(plane, f32),
            pltpu.VMEM((STEPS + 1,) + plane, f32),
            pltpu.VMEM((STEPS,) + plane, f32),
            pltpu.VMEM((STEPS,) + plane, f32),
            dma((4,)),
            dma((3,)),
            dma((2 + STEPS,)),
            dma((6,)),
            dma((2 if far == 1 else 4,)),
        ],
        compiler_params=pltpu.CompilerParams(collective_id=0, has_side_effects=True, vmem_limit_bytes=8 * 1024 * 1024),
    )(
        *[
            pltpu.with_memory_space_constraint(x, pltpu.HBM)
            for x in (
                flat(block_values, tiles), block_cols, flat(coarse_rhs, tiles), flat(guess, tiles),
            )
        ],
        bound_low, bound_high,
    )
    smoothed, residual, rms = pl.pallas_call(
        put_out,
        out_shape=(
            jax.ShapeDtypeStruct(plane, f32),
            jax.ShapeDtypeStruct(plane, f32),
            jax.ShapeDtypeStruct((1, LANES), f32),
        ),
        in_specs=[anywhere] * 3,
        out_specs=(anywhere,) * 3,
        scratch_shapes=[dma((3,))],
        compiler_params=pltpu.CompilerParams(vmem_limit_bytes=8 * 1024 * 1024),
    )(smoothed, residual, rms)
    return unflat(smoothed, comp), unflat(residual, comp), rms[0,:1]


def solution(mesh):
    split = ("sub", "agg")
    return jax.shard_map(
        functools.partial(shards, mesh.shape["sub"], mesh.shape["agg"]),
        mesh=mesh,
        in_specs=(
            P(None, None, None, split),
            P(None, split),
            P(None, split),
            P(None, split),
            P(),
            P(),
        ),
        out_specs=(P(None, split), P(None, split), P()),
        check_vma=False,
    )
```
